32 devices in a mesh: struct: 4 (over y, x), fluid: 8 (over z, core).
Axes of the slice: x: 2, y: 2, z: 4, core: 2. Of those that a mesh axis runs over, the one named last changes fastest.
Arguments:
- shell_motion: float32 [3, 262144], P(None, ('struct', 'fluid')), may hold values from -6 to 6
- owner: int32 [262144, 1], P(('struct', 'fluid')), may hold values from 0 to 31; in each aligned block of 8192 rows (0 to 8191, 8192 to 16383, ...) at most 512 rows name the same one
- stencil_slot: int32 [4, 8, 64, 128], P(None, 'struct', 'fluid'), may hold values from 0 to 16383
- stencil_weight: float32 [4, 8, 64, 128], P(None, 'struct', 'fluid'), may hold values from 0 to 0.5
- prev_motion: float32 [3, 8, 64, 256], P(None, 'struct', 'fluid'), may hold values from -6 to 6
- node_offset: float32 [3, 8, 64, 256], P(None, 'struct', 'fluid'), may hold values from -0.07 to 0.07
- cell_split: int32 [8, 64, 256], P('struct', 'fluid'), may hold values from 0 to 3
Outputs:
- mesh_motion: float32 [3, 8, 64, 256], P(None, 'struct', 'fluid')
The draws below stay inside these ranges and needn't reach their ends.
Inputs may be any that keep to these rules, and one draw needn't show every extreme that they name: Among the 8192 shell nodes of one device, no owner is named by more than 512 of them, a bound that some block reaches.
All inputs are finite; a program needn't handle non-finite values.
Results may differ from the reference program's by a relative error of at most 0.0003.
Values sent between devices are 32-bit elements; how exact they have to be, the bound alone decides.
A program may use at most 64 MiB of HBM per device.

```python
import math
from functools import partial
from functools import reduce
import jax
import jax.numpy as jnp
import numpy as np
from jax import lax

CY = 2
CZ = 8
NX = 256
IF_DEV = 8192
WALL = 128
STENCIL = 4
SWEEPS = 4
NY = 8
NZ = 64
NIF = 262144
CAP = 512
SLOTS = 16384
N_STRUCT = 4
N_FLUID = 8
DEVICES = 32


def with_ends(values, key, smallest, high):
    extent = values.shape
    place = [jax.random.randint(jax.random.fold_in(key, axis), (), 0, extent[axis]) for axis in range(len(extent))]
    values = values.at[tuple(place)].set(smallest)
    longest = extent.index(max(extent))
    place[longest] = (place[longest] + 1) % extent[longest]
    return values.at[tuple(place)].set(high)


def shard_levels(own_key, extent, shards, smallest, largest):
    def one(axis_at, blocks):
        heights = jax.random.uniform(jax.random.fold_in(jax.random.fold_in(own_key, 6), axis_at), (blocks,), jnp.float32, smallest / len(shards), largest / len(shards))
        return jnp.repeat(jnp.exp(heights), extent[axis_at] // blocks).reshape((-1,) + (1,) * (len(extent) - axis_at - 1))

    factor_of = one(*shards[0])
    for cut in shards[1:]:
        factor_of = factor_of * one(*cut)
    return factor_of


def deal_out(key, own, number, rows, amount, top, reach, lean):
    ranking = jax.random.permutation(key, amount)
    heavy_load, usual = load_shares(amount, rows * top, reach, lean, True), load_shares(amount, rows * top, reach, lean, False)
    places = jnp.arange(amount)

    def named(sizes, turn):
        used = int((sizes > 0).sum())
        fixed = max(1, used // 4)
        passed = fixed + (places - fixed + turn * (used - fixed)) % max(1, amount - fixed)
        return jnp.zeros((amount,), jnp.int32).at[ranking[jnp.where(places < fixed, places, passed)]].set(jnp.asarray(sizes, jnp.int32))

    sizes = jnp.where(number % 4 == 0, named(heavy_load, number // 4), named(usual, number - number // 4 - 1))
    mixed = jax.random.permutation(jax.random.fold_in(own, 3), amount)
    giver, receiver = mixed[0:amount // 2 * 2:2], mixed[1:amount // 2 * 2:2]
    room = jnp.minimum(sizes[giver] - 1, reach - sizes[receiver]) // 2
    room = jnp.where((giver == ranking[0]) | (receiver == ranking[0]) | (sizes[receiver] == 0), 0, jnp.maximum(room, 0))
    passed = jax.random.randint(jax.random.fold_in(own, 4), (amount // 2,), 0, 1 << 20) % (room + 1)
    sizes = sizes.at[giver].add(-passed).at[receiver].add(passed)
    items = jnp.searchsorted(jnp.cumsum(sizes), jnp.arange(rows * top), side="right").astype(jnp.int32)
    table = items.reshape(top, rows).T
    table = table[jax.random.permutation(jax.random.fold_in(own, 1), rows)]
    turn = jax.random.randint(jax.random.fold_in(own, 2), (rows, 1), 0, top)
    return jnp.take_along_axis(table, (jnp.arange(top)[None, :] + turn) % top, axis=1)


def load_shares(count, total, limit, slope, full):
    loads = [(1 << 20) // math.isqrt(standing ** slope) + 1 for standing in range(1, count + 1)]
    largest = limit if full else min(limit, max(-(-total // count), total * loads[0] // sum(loads)))
    least = 1 if total - largest >= count - 1 else 0
    given, surplus = [largest] + [least] * (count - 1), total - largest - least * (count - 1)
    while surplus > 0:
        free = [i for i in range(1, count) if given[i] < largest] or [i for i in range(1, count) if given[i] < limit]
        pool, left = sum([loads[i] for i in free]), surplus
        for i in free:
            more = min(limit - given[i], max(1, left * loads[i] // pool), surplus)
            given[i] = given[i] + more
            surplus = surplus - more
    return np.array(given)


def normal_values(stream_key, dims, deviation, most, cuts=(), kind=jnp.bfloat16):
    gain = shard_levels(stream_key, dims, cuts, -0.22, 0.18) if cuts else 1.0
    array = jax.random.normal(stream_key, dims, jnp.float32) * deviation * gain
    return jnp.minimum(jnp.maximum(array, -most), most).astype(kind)


def setup_inputs(seed: int = 0) -> dict:
    key_of = jax.random.split(jax.random.key(seed), 8)
    shell_motion = normal_values(key_of[0], (3, NIF), 1.0, 6.0, ((1, 32),), jnp.float32)
    owner_keys = jax.random.split(jax.random.fold_in(key_of[1], 1), NIF // IF_DEV)
    owner_turns = jax.random.permutation(jax.random.fold_in(key_of[1], 3), NIF // IF_DEV)
    owner = jax.vmap(lambda own, number: deal_out(jax.random.fold_in(key_of[1], 2), own, number, IF_DEV, DEVICES, 1, CAP, 2))(owner_keys, owner_turns).reshape((NIF, 1))
    stencil_slot = with_ends(jax.random.randint(key_of[2], (STENCIL, NY, NZ, WALL), 0, SLOTS), jax.random.fold_in(key_of[2], 1), 0, SLOTS - 1).astype(jnp.int32)
    stencil_weight = jnp.clip(0.5 * jax.random.uniform(key_of[3], (STENCIL, NY, NZ, WALL), jnp.float32) ** shard_levels(key_of[3], (STENCIL, NY, NZ, WALL), ((1, 4), (2, 8)), -0.2, 0.2), 0.0, 0.5)
    prev_motion = normal_values(key_of[4], (3, NY, NZ, NX), 1.0, 6.0, ((1, 4), (2, 8)), jnp.float32)
    node_offset = jnp.clip(jax.random.uniform(key_of[5], (3, NY, NZ, NX), jnp.float32, -0.07, 0.07) * shard_levels(key_of[5], (3, NY, NZ, NX), ((1, 4), (2, 8)), -0.4, 0.0), -0.07, 0.07)
    cell_split = with_ends(jax.random.randint(key_of[6], (NY, NZ, NX), 0, 4), jax.random.fold_in(key_of[6], 1), 0, 3).astype(jnp.int32)
    return dict(shell_motion=shell_motion, owner=owner, stencil_slot=stencil_slot, stencil_weight=stencil_weight, prev_motion=prev_motion, node_offset=node_offset, cell_split=cell_split)


LAMBDA_RATIO = 1.0
RELAX_FACTOR = 0.5
STEP_ORDERS = ((0, 1, 2), (0, 2, 1), (1, 0, 2), (1, 2, 0), (2, 0, 1), (2, 1, 0))
CORNER_LIST = tuple((shift_x, shift_y, shift_z) for shift_x in (0, 1) for shift_y in (0, 1) for shift_z in (0, 1))


def cross_product(left_vec, right_vec):
    return jnp.stack([left_vec[1] * right_vec[2] - left_vec[2] * right_vec[1],
                      left_vec[2] * right_vec[0] - left_vec[0] * right_vec[2],
                      left_vec[0] * right_vec[1] - left_vec[1] * right_vec[0]])


def select_flip(flip_y, flip_z, unflipped, flipped_z, flipped_y, flipped_both):
    return jnp.where(flip_y, jnp.where(flip_z, flipped_both, flipped_y), jnp.where(flip_z, flipped_z, unflipped))


def reflect_corners(corners, flip_y, flip_z):
    result = {}
    for corner in CORNER_LIST:
        shift_x, shift_y, shift_z = corner
        result[corner] = select_flip(flip_y, flip_z, corners[corner], corners[(shift_x, shift_y, 1 - shift_z)],
                                     corners[(shift_x, 1 - shift_y, shift_z)], corners[(shift_x, 1 - shift_y, 1 - shift_z)])
    return result


def flip_masks(split_codes):
    flip_y = (split_codes // 2) == 1
    flip_z = (split_codes % 2) == 1
    sign_y = jnp.where(flip_y, -1.0, 1.0).astype(jnp.float32)
    sign_z = jnp.where(flip_z, -1.0, 1.0).astype(jnp.float32)
    return flip_y, flip_z, sign_y, sign_z


def lattice_edge(vertex, sign_y, sign_z):
    return jnp.stack([jnp.full_like(sign_y, float(vertex[0])), sign_y * vertex[1], sign_z * vertex[2]])


def element_gradients(offsets, step_order, sign_y, sign_z):
    position = [0, 0, 0]
    vertex_path = [(0, 0, 0)]
    for axis_id in step_order:
        position[axis_id] = 1
        vertex_path.append(tuple(position))
    anchor = offsets[vertex_path[0]]
    edge_list = [lattice_edge(vertex, sign_y, sign_z) + offsets[vertex] - anchor for vertex in vertex_path[1:]]
    across_one = cross_product(edge_list[1], edge_list[2])
    across_two = cross_product(edge_list[2], edge_list[0])
    across_three = cross_product(edge_list[0], edge_list[1])
    volume_six = jnp.sum(edge_list[0] * across_one, axis=0)
    grad_one = across_one / volume_six
    grad_two = across_two / volume_six
    grad_three = across_three / volume_six
    grad_zero = -(grad_one + grad_two + grad_three)
    return vertex_path, [grad_zero, grad_one, grad_two, grad_three]


def element_forces(offsets, displace, sign_y, sign_z):
    forces = {corner: jnp.zeros_like(displace[corner]) for corner in CORNER_LIST}
    for step_order in STEP_ORDERS:
        vertex_path, gradient_list = element_gradients(offsets, step_order, sign_y, sign_z)
        tensor = displace[vertex_path[0]][:, None] * gradient_list[0][None, :]
        for vertex in range(1, 4):
            tensor = tensor + displace[vertex_path[vertex]][:, None] * gradient_list[vertex][None, :]
        trace_sum = tensor[0, 0] + tensor[1, 1] + tensor[2, 2]
        symmetric = tensor + jnp.swapaxes(tensor, 0, 1)
        for vertex in range(4):
            gradient = gradient_list[vertex]
            nodal_force = LAMBDA_RATIO * trace_sum * gradient + jnp.sum(symmetric * gradient[None, :], axis=1)
            forces[vertex_path[vertex]] = forces[vertex_path[vertex]] + nodal_force
    return forces


def element_diagonal(offsets, sign_y, sign_z):
    result = {corner: jnp.zeros_like(offsets[corner]) for corner in CORNER_LIST}
    for step_order in STEP_ORDERS:
        vertex_path, gradient_list = element_gradients(offsets, step_order, sign_y, sign_z)
        for vertex in range(4):
            gradient = gradient_list[vertex]
            entry = (LAMBDA_RATIO + 1.0) * gradient * gradient + jnp.sum(gradient * gradient, axis=0)
            result[vertex_path[vertex]] = result[vertex_path[vertex]] + entry
    return result


def row_corners(lower, upper):
    return {corner: jnp.roll(upper if corner[1] else lower, (-corner[2], -corner[0]), axis=(-2, -1)) for corner in CORNER_LIST}


def row_assemble(per_corner):
    lower_part = reduce(jnp.add, [jnp.roll(per_corner[corner], (corner[2], corner[0]), axis=(-2, -1)) for corner in CORNER_LIST if corner[1] == 0])
    upper_part = reduce(jnp.add, [jnp.roll(per_corner[corner], (corner[2], corner[0]), axis=(-2, -1)) for corner in CORNER_LIST if corner[1] == 1])
    return lower_part, upper_part


def combine_rows(pair):
    lower_part, upper_part = pair
    return jnp.transpose(lower_part + jnp.roll(upper_part, 1, axis=0), (1, 0, 2, 3))


def row_slices(nodal_field, row_index):
    lower = lax.dynamic_index_in_dim(nodal_field, row_index, 1, keepdims=False)
    upper = lax.dynamic_index_in_dim(nodal_field, (row_index + 1) % NY, 1, keepdims=False)
    return row_corners(lower, upper)


def row_masks(cell_split, row_index):
    return flip_masks(lax.dynamic_index_in_dim(cell_split, row_index, 0, keepdims=False))


def diagonal_row(node_offset, cell_split, row_index):
    flip_y, flip_z, sign_y, sign_z = row_masks(cell_split, row_index)
    offsets = reflect_corners(row_slices(node_offset, row_index), flip_y, flip_z)
    return row_assemble(reflect_corners(element_diagonal(offsets, sign_y, sign_z), flip_y, flip_z))


def force_row(node_offset, cell_split, current, row_index):
    flip_y, flip_z, sign_y, sign_z = row_masks(cell_split, row_index)
    offsets = reflect_corners(row_slices(node_offset, row_index), flip_y, flip_z)
    displace = reflect_corners(row_slices(current, row_index), flip_y, flip_z)
    return row_assemble(reflect_corners(element_forces(offsets, displace, sign_y, sign_z), flip_y, flip_z))


def reference(shell_motion, owner, stencil_slot, stencil_weight, prev_motion, node_offset, cell_split):
    devices = N_STRUCT * N_FLUID
    slot_count = devices * CAP
    targets = jnp.arange(devices, dtype=jnp.int32)

    def pack_source(source):
        owner_rows = lax.dynamic_slice_in_dim(owner[:, 0], source * IF_DEV, IF_DEV)
        values = lax.dynamic_slice_in_dim(shell_motion, source * IF_DEV, IF_DEV, 1)
        onehot = (owner_rows[:, None] == targets[None, :]).astype(jnp.int32)
        before = jnp.cumsum(onehot, axis=0) - onehot
        slot_rank = jnp.sum(before * onehot, axis=1)
        slot_place = (owner_rows * CAP + slot_rank).astype(jnp.int32)
        return jnp.zeros((3, slot_count), dtype=shell_motion.dtype).at[:, slot_place].set(values)

    packed = lax.map(pack_source, targets)
    received = packed.reshape(devices, 3, devices, CAP).transpose(1, 2, 0, 3).reshape(3, devices * slot_count)
    row_owner = (jnp.arange(NY, dtype=jnp.int32) // CY) * N_FLUID
    column_owner = jnp.arange(NZ, dtype=jnp.int32) // CZ
    holder = row_owner[:, None] + column_owner[None, :]
    flat_index = (holder[None, :, :, None] * slot_count + stencil_slot).astype(jnp.int32)
    gathered = jnp.take(received, flat_index.reshape(-1), axis=1).reshape(3, STENCIL, NY, NZ, WALL)
    wall_values = jnp.sum(stencil_weight[None] * gathered, axis=1)
    motion = jnp.concatenate([wall_values, prev_motion[:, :, :, WALL:]], axis=3)
    is_wall = (jnp.arange(NX, dtype=jnp.int32) < WALL)[None, None, None, :]
    rows_index = jnp.arange(NY, dtype=jnp.int32)
    diagonal = combine_rows(lax.map(partial(diagonal_row, node_offset, cell_split), rows_index))
    for sweep_index in range(SWEEPS):
        forces = combine_rows(lax.map(partial(force_row, node_offset, cell_split, motion), rows_index))
        motion = jnp.where(is_wall, motion, motion - RELAX_FACTOR * forces / diagonal)
    return motion
```

```python
import functools

import jax
import jax.numpy as jnp
from jax import lax
from jax.experimental import pallas as pl
from jax.experimental.pallas import tpu as pltpu
from jax.sharding import PartitionSpec as P

SWEEPS = 4
LANES = 128
LAMBDA_RATIO = 1.0
RELAX_FACTOR = 0.5
STEP_ORDERS = ((0, 1, 2), (0, 2, 1), (1, 0, 2), (1, 2, 0), (2, 0, 1), (2, 1, 0))
CORNERS = tuple((a, b, c) for a in (0, 1) for b in (0, 1) for c in (0, 1))
COLUMNS = 16
MESH = pl.DeviceIdType.MESH
BF16 = jnp.bfloat16
F32 = jnp.float32


def split_two(values):
    high = values.astype(BF16)
    low = (values - high.astype(F32)).astype(BF16)
    return high, low


def iota(shape, dim):
    return lax.broadcasted_iota(jnp.int32, shape, dim)


def swap_corners(corners, flip_y, flip_z):
    middle = {}
    for a, b, c in CORNERS:
        middle[a, b, c] = [
            jnp.where(flip_y, q, p) for p, q in zip(corners[a, b, c], corners[a, 1 - b, c])
        ]
    return {
        (a, b, c): [jnp.where(flip_z, q, p) for p, q in zip(middle[a, b, c], middle[a, b, 1 - c])]
        for a, b, c in CORNERS
    }


def paths():
    for order in STEP_ORDERS:
        position, path = [0, 0, 0], []
        for axis_id in order:
            position[axis_id] = 1
            path.append(tuple(position))
        yield path


def cross(p, q):
    return [p[1] * q[2] - p[2] * q[1], p[2] * q[0] - p[0] * q[2], p[0] * q[1] - p[1] * q[0]]


def add_to(table, key, vector):
    table[key] = [p + q for p, q in zip(table[key], vector)] if key in table else list(vector)


def cell_gradients(offsets, flip_y, flip_z):
    offsets = swap_corners(offsets, flip_y, flip_z)
    sign_y, sign_z = jnp.where(flip_y, -1.0, 1.0), jnp.where(flip_z, -1.0, 1.0)
    anchor = offsets[0, 0, 0]
    edges = {}
    for vertex in CORNERS[1:]:
        edge = [p - q for p, q in zip(offsets[vertex], anchor)]
        if vertex[0]:
            edge[0] = edge[0] + 1.0
        if vertex[1]:
            edge[1] = edge[1] + sign_y
        if vertex[2]:
            edge[2] = edge[2] + sign_z
        edges[vertex] = edge
    gradients, diagonal = [], {}
    for path in paths():
        one, two, three = [edges[v] for v in path]
        across = [cross(two, three), cross(three, one), cross(one, two)]
        volume = one[0] * across[0][0] + one[1] * across[0][1] + one[2] * across[0][2]
        inverse = 1.0 / volume
        grads = [[p * inverse for p in vector] for vector in across]
        gradients.append(grads)
        first = [-(grads[0][p] + grads[1][p] + grads[2][p]) for p in range(3)]
        for vertex, grad in zip([(0, 0, 0)] + path, [first] + grads):
            square = [p * p for p in grad]
            norm = square[0] + square[1] + square[2]
            add_to(diagonal, vertex, [(LAMBDA_RATIO + 1.0) * p + norm for p in square])
    return gradients, swap_corners(diagonal, flip_y, flip_z)


def cell_forces(gradients, motion, flip_y, flip_z):
    motion = swap_corners(motion, flip_y, flip_z)
    anchor = motion[0, 0, 0]
    moves = {v: [p - q for p, q in zip(motion[v], anchor)] for v in CORNERS[1:]}
    forces = {}
    for tet, path in enumerate(paths()):
        grads = [[gradients(tet, v, p) for p in range(3)] for v in range(3)]
        tensor = [
            [
                moves[path[0]][p] * grads[0][q]
                + moves[path[1]][p] * grads[1][q]
                + moves[path[2]][p] * grads[2][q]
                for q in range(3)
            ]
            for p in range(3)
        ]
        trace = LAMBDA_RATIO * (tensor[0][0] + tensor[1][1] + tensor[2][2])
        stress = [[None] * 3 for _ in range(3)]
        for p in range(3):
            stress[p][p] = tensor[p][p] + tensor[p][p] + trace
            for q in range(p):
                stress[p][q] = stress[q][p] = tensor[p][q] + tensor[q][p]
        for v in range(3):
            add_to(
                forces,
                path[v],
                [
                    stress[p][0] * grads[v][0] + stress[p][1] * grads[v][1] + stress[p][2] * grads[v][2]
                    for p in range(3)
                ],
            )
    first = None
    for vector in forces.values():
        first = vector if first is None else [p + q for p, q in zip(first, vector)]
    forces[0, 0, 0] = [-p for p in first]
    return swap_corners(forces, flip_y, flip_z)


def turn(x, shift, axis):
    shift %= x.shape[axis]
    return pltpu.roll(x, shift, axis) if shift else x


def float_codes(value):
    return value >= 1.5, (value == 1.0) | (value == 3.0)


def int_codes(value):
    return value >= 2, (value & 1) == 1


def corners_of(low, high):
    corners = {}
    for b, row in ((0, low), (1, high)):
        for a in (0, 1):
            far = [turn(p, -a, 1) for p in row]
            corners[a, b, 0] = far
            corners[a, b, 1] = [turn(p, -1, 0) for p in far]
    return corners


def assemble_row(parts, b):
    near = [p + turn(q, 1, 0) for p, q in zip(parts[0, b, 0], parts[0, b, 1])]
    far = [p + turn(q, 1, 0) for p, q in zip(parts[1, b, 0], parts[1, b, 1])]
    return [p + turn(q, 1, 1) for p, q in zip(near, far)]


def merge_planes(left, own, right, depth):
    return jnp.concatenate([left[left.shape[0] - depth :], own, right[:depth]], axis=0)


def place_nodes(devices, capacity, own_ref, place_ref):
    rows = own_ref.shape[0]
    own = own_ref[...]
    upper = (iota((LANES, LANES), 0) < iota((LANES, LANES), 1)).astype(F32)
    prefix_all = jnp.concatenate([upper, jnp.ones((LANES, LANES), F32)], axis=1).astype(BF16)
    lower = (iota((rows, rows), 1) < iota((rows, rows), 0)).astype(F32).astype(BF16)
    chunk = min(devices, 32)

    def ranks(step, place):
        for o in range(chunk):
            target = step * chunk + o
            named = own == target
            both = jnp.dot(named.astype(F32).astype(BF16), prefix_all, preferred_element_type=F32)
            ahead = jnp.dot(lower, both[:, LANES:].astype(BF16), preferred_element_type=F32)
            rank = (both[:, :LANES] + ahead).astype(jnp.int32)
            place = jnp.where(named, rank + target * capacity, place)
        return place

    place = jnp.zeros((rows, LANES), jnp.int32)
    if chunk == devices:
        place = ranks(0, place)
    else:
        place = lax.fori_loop(0, devices // chunk, ranks, place)
    place_ref[...] = place


def pack_nodes(first, last, place_ref, val_ref, acc_ref):
    wide = 2 * LANES
    groups = acc_ref.shape[0] // 3
    group_id = iota((groups, LANES), 0)
    lane_id = iota((wide, LANES), 0)

    def spread(step, carry):
        total = None
        for u in range(4):
            row = step * 4 + u
            at = place_ref[pl.ds(row, 1), :]
            hit = group_id == at // wide
            column = (lane_id == at % wide).astype(F32).astype(BF16)
            parts = []
            for c in range(3):
                value = val_ref[pl.ds(c, 1), pl.ds(pl.multiple_of(row * LANES, LANES), LANES)]
                high = value.astype(BF16).astype(F32)
                low = value - high
                parts.append(
                    jnp.concatenate(
                        [jnp.where(hit, high, 0.0).astype(BF16), jnp.where(hit, low, 0.0).astype(BF16)],
                        axis=1,
                    )
                )
            left = jnp.concatenate(parts, axis=0)
            right = jnp.concatenate([column, column], axis=1)
            product = lax.dot_general(
                left, right, (((1,), (1,)), ((), ())), preferred_element_type=F32
            )
            total = product if total is None else total + product
        acc_ref[...] += total
        return carry

    lax.fori_loop(first, last, spread, 0)


def window_kernel(
    counts,
    shell,
    owner,
    slot,
    weight,
    prev,
    offset,
    split,
    out,
    v_shell,
    v_owner,
    v_slot,
    v_weight,
    near_offset,
    near_split,
    near_motion,
    wall_offset,
    wall_split,
    place,
    acc,
    packed,
    received,
    table,
    both,
    v_wall,
    edge_in,
    wall_in,
    edge_field,
    edge_grad,
    edge_diag,
    edge_motion,
    motion,
    force,
    node_offset,
    cell_code,
    grad,
    diag,
    local_sem,
    near_send,
    near_recv,
    edge_send,
    edge_recv,
    row_send,
    row_recv,
    pack_send,
    pack_recv,
    wall_send,
    wall_recv,
):
    num_struct, num_fluid = counts
    devices = num_struct * num_fluid
    s, f = lax.axis_index("struct"), lax.axis_index("fluid")
    me = s * num_fluid + f
    stencil, count_y, count_z, wall = slot.shape
    free = prev.shape[3] - wall
    nodes = count_y * count_z
    deep = count_z + 2 * SWEEPS
    span = count_y * COLUMNS
    rows_own = v_owner.shape[0]
    capacity = 2 * rows_own * LANES // devices
    pieces = capacity // LANES
    groups = devices * pieces
    half = LANES // 2
    last_y = count_y - 1

    def peer(ds, df):
        return ((s + ds + num_struct) % num_struct, (f + df + num_fluid) % num_fluid)

    def remote(src, dst, send, recv, where):
        return pltpu.make_async_remote_copy(
            src_ref=src, dst_ref=dst, send_sem=send, recv_sem=recv, device_id=where, device_id_type=MESH
        )

    free_lanes, wall_lanes = pl.ds(wall, free), pl.ds(0, wall)
    loads = [
        (owner, v_owner),
        (offset.at[:, :, :, free_lanes], near_offset.at[4]),
        (split.at[:, :, free_lanes], near_split.at[4]),
        (prev.at[:, :, :, free_lanes], near_motion.at[4]),
        (offset.at[:, :, :, wall_lanes], wall_offset),
        (split.at[:, :, wall_lanes], wall_split),
        (shell, v_shell),
        (slot, v_slot),
        (weight, v_weight),
    ]
    loads = [pltpu.make_async_copy(a, b, local_sem.at[n]) for n, (a, b) in enumerate(loads)]
    for load in loads:
        load.start()

    barrier = pltpu.get_barrier_semaphore()

    def greet(d, carry):
        other = (me + d) % devices
        pl.semaphore_signal(
            barrier, inc=1, device_id=(other // num_fluid, other % num_fluid), device_id_type=MESH
        )
        return carry

    lax.fori_loop(1, devices, greet, 0)

    loads[0].wait()
    place_nodes(devices, capacity, v_owner, place)
    for load in loads[1:6]:
        load.wait()

    lane8 = iota((count_z, LANES), 1)
    own_tiles = [jnp.zeros((count_z, LANES), F32) for _ in range(4)]
    for n in range(7):
        for j in range(count_y):
            if n < 3:
                a, w = near_offset[4, n, j], wall_offset[n, j]
            elif n == 3:
                a, w = near_split[4, j].astype(F32), wall_split[j].astype(F32)
            else:
                a = near_motion[4, n - 4, j]
                w = a
            for side in (0, 1):
                base = half * (n % 2) + span * side + COLUMNS * j
                if side == 0:
                    joined = turn(jnp.where(lane8 == LANES - 1, w, a), base + 1, 1)
                else:
                    joined = turn(jnp.where(lane8 == 0, w, a), base + 2 * SWEEPS, 1)
                inside = (lane8 >= base) & (lane8 < base + COLUMNS)
                own_tiles[n // 2] = jnp.where(inside, joined, own_tiles[n // 2])
    for n in range(4):
        edge_in[0, 1, n] = own_tiles[n]

    pl.semaphore_wait(barrier, devices - 1)

    def near_copies(ds, df, at):
        src, dst = 4, (1 - ds) * 3 + 1 - df
        if at is not None:
            dst = at
        lines = pl.ds(0, count_y) if ds == 0 else pl.ds(last_y if ds > 0 else 0, 1)
        if at is not None and ds != 0:
            lines = pl.ds(last_y if ds < 0 else 0, 1)
        send = (ds + 1) * 3 + df + 1
        return [
            remote(
                near_offset.at[src, :, lines],
                near_offset.at[dst, :, lines],
                near_send.at[send, 0],
                near_recv.at[dst, 0],
                peer(ds, df),
            ),
            remote(
                near_split.at[src, lines],
                near_split.at[dst, lines],
                near_send.at[send, 1],
                near_recv.at[dst, 1],
                peer(ds, df),
            ),
            remote(
                near_motion.at[src, :, lines],
                near_motion.at[dst, :, lines],
                near_send.at[send, 2],
                near_recv.at[dst, 2],
                peer(ds, df),
            ),
        ]

    around = [(ds, df) for ds in (-1, 0, 1) for df in (-1, 0, 1) if (ds, df) != (0, 0)]
    near_out = [copy for ds, df in around for copy in near_copies(ds, df, None)]
    near_back = [copy for ds, df in around for copy in near_copies(ds, df, (ds + 1) * 3 + df + 1)]
    for copy in near_out:
        copy.start()

    wide_around = [(r, df) for r in range(num_struct) for df in (-1, 0, 1) if (r, df) != (0, 0)]

    def wide_copies(buffer, send, recv):
        return [
            remote(
                buffer.at[0, 1],
                buffer.at[r, df + 1],
                send.at[r * 3 + df + 1],
                recv.at[r * 3 + df + 1],
                peer(-r, -df),
            )
            for r, df in wide_around
        ]

    edge_copies = wide_copies(edge_in, edge_send, edge_recv)
    for copy in edge_copies:
        copy.start()

    def row_copies(sweep):
        return [
            remote(motion.at[sweep, 1], motion.at[sweep, 3], row_send.at[sweep, 0], row_recv.at[sweep, 0], peer(-1, 0)),
            remote(motion.at[sweep, 2], motion.at[sweep, 0], row_send.at[sweep, 1], row_recv.at[sweep, 1], peer(1, 0)),
        ]

    def prepare_main():
        for r in range(count_y + 2):
            ds, j = (-1, last_y) if r == 0 else (1, 0) if r == count_y + 1 else (0, r - 1)
            at = [(ds + 1) * 3 + df + 1 for df in (-1, 0, 1)]
            for c in range(3):
                node_offset[r, c] = merge_planes(*[near_offset[n, c, j] for n in at], SWEEPS)
                motion[0, r, c] = merge_planes(*[near_motion[n, c, j] for n in at], SWEEPS)
            cell_code[r] = merge_planes(*[near_split[n, j] for n in at], SWEEPS)
        diag[...] = jnp.zeros_like(diag)

        def row(j, carry):
            flip_y, flip_z = int_codes(cell_code[j])
            corners = corners_of(
                [node_offset[j, c] for c in range(3)], [node_offset[j + 1, c] for c in range(3)]
            )
            gradients, parts = cell_gradients(corners, flip_y, flip_z)
            for tet in range(6):
                for v in range(3):
                    for p in range(3):
                        grad[j, 9 * tet + 3 * v + p] = gradients[tet][v][p]
            for b in (0, 1):
                for c, value in enumerate(assemble_row(parts, b)):
                    diag[j + b, c] = diag[j + b, c] + value
            return carry

        lax.fori_loop(0, count_y + 1, row, 0)

    def sweep_main(sweep):
        force[...] = jnp.zeros_like(force)

        def row(j, carry):
            flip_y, flip_z = int_codes(cell_code[j])
            corners = corners_of(
                [motion[sweep, j, c] for c in range(3)], [motion[sweep, j + 1, c] for c in range(3)]
            )
            parts = cell_forces(lambda tet, v, p: grad[j, 9 * tet + 3 * v + p], corners, flip_y, flip_z)
            for b in (0, 1):
                for c, value in enumerate(assemble_row(parts, b)):
                    force[j + b, c] = force[j + b, c] + value
            return carry

        lax.fori_loop(0, count_y + 1, row, 0)
        for r in range(1, count_y + 1):
            for c in range(3):
                motion[sweep + 1, r, c] = motion[sweep, r, c] - RELAX_FACTOR * force[r, c] / diag[r, c]

    lane_deep = iota((deep, LANES), 1)
    lane_edge = iota((2 * deep, LANES), 1)

    def wide_merge(read):
        return [merge_planes(read(r, 0), read(r, 1), read(r, 2), SWEEPS) for r in range(num_struct)]

    def edge_corners(values):
        corners = {}
        for a in (0, 1):
            for b in (0, 1):
                shifted = [turn(p, -a - COLUMNS * b, 1) for p in values]
                corners[a, b, 0] = shifted
                corners[a, b, 1] = [turn(p, -1, 0) for p in shifted]
        return corners

    def edge_assemble(parts):
        low, high = assemble_row(parts, 0), assemble_row(parts, 1)
        return [p + turn(q, COLUMNS, 1) for p, q in zip(low, high)]

    def prepare_edge():
        for tile in range(4):
            merged = wide_merge(lambda r, d: edge_in[r, d, tile])
            for n in (2 * tile, 2 * tile + 1):
                if n == 7:
                    continue
                for side in (0, 1):
                    base = half * (n % 2) + span * side
                    total = None
                    for r in range(num_struct):
                        moved = turn(merged[r], span * r - base, 1)
                        total = moved if total is None else jnp.where(lane_deep >= span * r, moved, total)
                    edge_field[n, pl.ds(deep * side, deep), :] = total
        flip_y, flip_z = float_codes(edge_field[3])
        gradients, parts = cell_gradients(edge_corners([edge_field[c] for c in range(3)]), flip_y, flip_z)
        for tet in range(6):
            for v in range(3):
                for p in range(3):
                    edge_grad[9 * tet + 3 * v + p] = gradients[tet][v][p]
        for c, value in enumerate(edge_assemble(parts)):
            edge_diag[c] = value

    def plane_points(ref, zero):
        row, lane = iota((nodes, LANES), 0), iota((nodes, LANES), 1)
        within = row // count_z * (2 * count_z) + count_z - 1 - row % count_z
        total = None
        for t in range(stencil):
            whole = jnp.concatenate([ref[t, j] for j in range(count_y)], axis=0)
            for side in (0, 1):
                column = wall - 1 if side == 0 else 0
                spread = jnp.broadcast_to(whole[:, column : column + 1], (nodes, LANES))
                part = jnp.where(lane == 2 * nodes * t + count_z * side + within, spread, zero)
                total = part if total is None else total + part
        return jnp.sum(total, axis=0, keepdims=True)

    acc[...] = jnp.zeros_like(acc)
    loads[6].wait()
    steps = rows_own // 4
    pack_nodes(0, steps // 2, place, v_shell, acc)
    for copy in near_back:
        copy.wait_recv()
    prepare_main()
    sweep_main(0)
    for copy in row_copies(1):
        copy.start()
    pack_nodes(steps // 2, steps, place, v_shell, acc)
    pack_groups = groups // 2
    for o in range(devices):
        for c in range(3):
            for b in range(pieces):
                m = o * pieces + b
                packed[o, pl.ds(c * pieces + b, 1), :] = acc[
                    pl.ds(c * pack_groups + m // 2, 1), pl.ds((m % 2) * LANES, LANES)
                ]

    def pack_copy(other):
        return remote(
            packed.at[other],
            received.at[me],
            pack_send.at[other],
            pack_recv.at[me],
            (other // num_fluid, other % num_fluid),
        )

    def pack_arrival(other):
        return remote(
            packed.at[other],
            received.at[other],
            pack_send.at[other],
            pack_recv.at[other],
            (other // num_fluid, other % num_fluid),
        )

    def send_pack(d, carry):
        pack_copy((me + d) % devices).start()
        return carry

    lax.fori_loop(1, devices, send_pack, 0)
    received[me] = packed[me]

    for copy in edge_copies:
        copy.wait_recv()
    prepare_edge()
    for copy in row_copies(1):
        copy.wait_recv()
    sweep_main(1)
    for copy in row_copies(2):
        copy.start()
    loads[7].wait()
    loads[8].wait()
    plane_slot, plane_weight = plane_points(v_slot, 0), plane_points(v_weight, 0.0)
    for copy in row_copies(2):
        copy.wait_recv()
    sweep_main(2)
    for copy in row_copies(3):
        copy.start()

    def await_pack(d, carry):
        pack_arrival((me + d) % devices).wait_recv()
        return carry

    lax.fori_loop(1, devices, await_pack, 0)

    for c in range(3):
        for o in range(devices):
            table[pl.ds(c * groups + o * pieces, pieces), :] = received[o, pl.ds(c * pieces, pieces), :]
    high, low = split_two(table[...])
    both[:, :LANES] = high
    both[:, LANES:] = low

    pick = (iota((LANES, LANES), 0) == plane_slot % LANES).astype(F32).astype(BF16)
    found = jnp.dot(both[...], jnp.concatenate([pick, pick], axis=0), preferred_element_type=F32)
    scaled = jnp.where(iota((groups, LANES), 0) == plane_slot // LANES, plane_weight, 0.0)
    tile = jnp.zeros((count_z, LANES), F32)
    for c in range(3):
        line = jnp.sum(found[c * groups : (c + 1) * groups] * scaled, axis=0, keepdims=True)
        period = LANES // 2
        while period >= 2 * nodes:
            line = line + turn(line, period, 1)
            period //= 2
        spread = pltpu.roll(jnp.broadcast_to(line, (count_z, LANES)), 0, 1, stride=1, stride_axis=0)
        tile = jnp.where((lane8 >= span * c) & (lane8 < span * (c + 1)), spread, tile)
    wall_in[0, 1] = tile
    wall_copies = wide_copies(wall_in, wall_send, wall_recv)
    for copy in wall_copies:
        copy.start()

    wide = 2 * LANES
    lane_id = iota((LANES, wide), 0)
    group_id = iota((groups, wide), 0)

    def pair(step, carry):
        j, k = 2 * step // count_z, 2 * step % count_z
        sums = [None] * 3
        for t in range(stencil):
            at = jnp.concatenate(
                [v_slot[t, j, pl.ds(k, 1), :], v_slot[t, j, pl.ds(k + 1, 1), :]], axis=1
            )
            by = jnp.concatenate(
                [v_weight[t, j, pl.ds(k, 1), :], v_weight[t, j, pl.ds(k + 1, 1), :]], axis=1
            )
            choose = (lane_id == at % LANES).astype(F32).astype(BF16)
            values = jnp.dot(
                both[...], jnp.concatenate([choose, choose], axis=0), preferred_element_type=F32
            )
            factor = jnp.where(group_id == at // LANES, by, 0.0)
            for c in range(3):
                term = values[c * groups : (c + 1) * groups] * factor
                sums[c] = term if sums[c] is None else sums[c] + term
        for c in range(3):
            line = jnp.sum(sums[c], axis=0, keepdims=True)
            v_wall[c, pl.ds(2 * step, 1), :] = line[:, :LANES]
            v_wall[c, pl.ds(2 * step + 1, 1), :] = line[:, LANES:]
        return carry

    lax.fori_loop(0, nodes // 2, pair, 0)

    for copy in row_copies(3):
        copy.wait_recv()
    sweep_main(3)

    for copy in wall_copies:
        copy.wait_recv()
    column = lane_edge % COLUMNS
    second = iota((2 * deep, LANES), 0) >= deep
    wall_column = column == jnp.where(second, 2 * SWEEPS, 0)
    inner = (column >= 1) & (column < 2 * SWEEPS)
    arrived = wide_merge(lambda r, d: wall_in[r, d])
    for c in range(3):
        total = None
        for r in range(num_struct):
            moved = turn(arrived[r], span * (r - c) - (count_z - 1), 1)
            total = moved if total is None else jnp.where(lane_deep >= span * r, moved, total)
        total = jnp.concatenate([total, total], axis=0)
        edge_motion[c] = jnp.where(wall_column, total, edge_field[4 + c])

    def sweep_edge(step, carry):
        flip_y, flip_z = float_codes(edge_field[3])
        parts = cell_forces(
            lambda tet, v, p: edge_grad[9 * tet + 3 * v + p],
            edge_corners([edge_motion[c] for c in range(3)]),
            flip_y,
            flip_z,
        )
        for c, value in enumerate(edge_assemble(parts)):
            now = edge_motion[c]
            edge_motion[c] = jnp.where(inner, now - RELAX_FACTOR * value / edge_diag[c], now)
        return carry

    lax.fori_loop(0, SWEEPS, sweep_edge, 0)

    for c in range(3):
        for j in range(count_y):
            out[c, j, :, wall_lanes] = v_wall[c, pl.ds(j * count_z, count_z), :]
            main = motion[SWEEPS, j + 1, c, SWEEPS : SWEEPS + count_z, :]
            low = turn(edge_motion[c, SWEEPS : SWEEPS + count_z, :], -1 - COLUMNS * j, 1)
            high = turn(
                edge_motion[c, deep + SWEEPS : deep + SWEEPS + count_z, :],
                free - 2 * SWEEPS - COLUMNS * j,
                1,
            )
            main = jnp.where(lane8 < SWEEPS, low, jnp.where(lane8 >= free - SWEEPS, high, main))
            out[c, j, :, free_lanes] = main

    for copy in near_out + edge_copies + wall_copies:
        copy.wait_send()
    for sweep in range(1, SWEEPS):
        for copy in row_copies(sweep):
            copy.wait_send()

    def drain(d, carry):
        pack_copy((me + d) % devices).wait_send()
        return carry

    lax.fori_loop(1, devices, drain, 0)


def shards(shell_motion, owner, stencil_slot, stencil_weight, prev_motion, node_offset, cell_split):
    num_struct, num_fluid = lax.axis_size("struct"), lax.axis_size("fluid")
    devices = num_struct * num_fluid
    own = shell_motion.shape[1]
    pieces = 2 * own // devices // LANES
    groups = devices * pieces
    stencil, count_y, count_z, wall = stencil_slot.shape
    free = prev_motion.shape[3] - wall
    nodes, deep = count_y * count_z, count_z + 2 * SWEEPS
    rows = count_y + 2
    assert wall == free == LANES and count_z == 8 and num_struct >= 3 and num_fluid >= 3
    assert num_struct * count_y * COLUMNS == LANES and 2 * stencil * nodes == LANES and count_y == 2
    vmem, dma = pltpu.VMEM, pltpu.SemaphoreType.DMA
    scratch = [
        vmem((3, own), F32),
        vmem((own // LANES, LANES), jnp.int32),
        vmem((stencil, count_y, count_z, wall), jnp.int32),
        vmem((stencil, count_y, count_z, wall), F32),
        vmem((9, 3, count_y, count_z, free), F32),
        vmem((9, count_y, count_z, free), jnp.int32),
        vmem((9, 3, count_y, count_z, free), F32),
        vmem((3, count_y, count_z, wall), F32),
        vmem((count_y, count_z, wall), jnp.int32),
        vmem((own // LANES, LANES), jnp.int32),
        vmem((3 * groups // 2, 2 * LANES), F32),
        vmem((devices, 3 * pieces, LANES), F32),
        vmem((devices, 3 * pieces, LANES), F32),
        vmem((3 * groups, LANES), F32),
        vmem((3 * groups, 2 * LANES), BF16),
        vmem((3, nodes, wall), F32),
        vmem((num_struct, 3, 4, count_z, LANES), F32),
        vmem((num_struct, 3, count_z, LANES), F32),
        vmem((7, 2 * deep, LANES), F32),
        vmem((54, 2 * deep, LANES), F32),
        vmem((3, 2 * deep, LANES), F32),
        vmem((3, 2 * deep, LANES), F32),
        vmem((SWEEPS + 1, rows, 3, deep, free), F32),
        vmem((rows, 3, deep, free), F32),
        vmem((rows, 3, deep, free), F32),
        vmem((rows, deep, free), jnp.int32),
        vmem((rows - 1, 54, deep, free), F32),
        vmem((rows, 3, deep, free), F32),
        dma((9,)),
        dma((9, 3)),
        dma((9, 3)),
        dma((3 * num_struct,)),
        dma((3 * num_struct,)),
        dma((SWEEPS, 2)),
        dma((SWEEPS, 2)),
        dma((devices,)),
        dma((devices,)),
        dma((3 * num_struct,)),
        dma((3 * num_struct,)),
    ]
    return pl.pallas_call(
        functools.partial(window_kernel, (num_struct, num_fluid)),
        out_shape=jax.ShapeDtypeStruct(prev_motion.shape, F32),
        in_specs=[pl.BlockSpec(memory_space=pltpu.HBM)] * 7,
        out_specs=pl.BlockSpec(memory_space=pltpu.VMEM),
        scratch_shapes=scratch,
        cost_estimate=pl.CostEstimate(flops=4 << 30, bytes_accessed=16 << 20, transcendentals=0),
        compiler_params=pltpu.CompilerParams(
            collective_id=0, has_side_effects=True, vmem_limit_bytes=48 << 20
        ),
    )(
        shell_motion,
        owner.reshape(own // LANES, LANES),
        stencil_slot,
        stencil_weight,
        prev_motion,
        node_offset,
        cell_split,
    )


def solution(mesh):
    return jax.shard_map(
        shards,
        mesh=mesh,
        in_specs=(
            P(None, ("struct", "fluid")),
            P(("struct", "fluid"), None),
            P(None, "struct", "fluid", None),
            P(None, "struct", "fluid", None),
            P(None, "struct", "fluid", None),
            P(None, "struct", "fluid", None),
            P("struct", "fluid", None),
        ),
        out_specs=P(None, "struct", "fluid", None),
        check_vma=False,
    )
```

```python
import functools

import jax
import jax.numpy as jnp
from jax import lax
from jax.experimental import pallas as pl
from jax.experimental.pallas import tpu as pltpu
from jax.sharding import PartitionSpec as P

SWEEPS = 4
LANES = 128
LAMBDA_RATIO = 1.0
RELAX_FACTOR = 0.5
STEP_ORDERS = ((0, 1, 2), (0, 2, 1), (1, 0, 2), (1, 2, 0), (2, 0, 1), (2, 1, 0))
CORNERS = tuple((a, b, c) for a in (0, 1) for b in (0, 1) for c in (0, 1))
COLUMNS = 16
FIELDS = 8
ROW_STEP = 8
MESH = pl.DeviceIdType.MESH
BF16 = jnp.bfloat16
F32 = jnp.float32


def split_two(values):
    high = values.astype(BF16)
    low = (values - high.astype(F32)).astype(BF16)
    return high, low


def iota(shape, dim):
    return lax.broadcasted_iota(jnp.int32, shape, dim)


def swap_corners(corners, flip_y, flip_z):
    middle = {}
    for a, b, c in CORNERS:
        middle[a, b, c] = [
            jnp.where(flip_y, q, p) for p, q in zip(corners[a, b, c], corners[a, 1 - b, c])
        ]
    return {
        (a, b, c): [jnp.where(flip_z, q, p) for p, q in zip(middle[a, b, c], middle[a, b, 1 - c])]
        for a, b, c in CORNERS
    }


def paths():
    for order in STEP_ORDERS:
        position, path = [0, 0, 0], []
        for axis_id in order:
            position[axis_id] = 1
            path.append(tuple(position))
        yield path


def cross(p, q):
    return [p[1] * q[2] - p[2] * q[1], p[2] * q[0] - p[0] * q[2], p[0] * q[1] - p[1] * q[0]]


def add_to(table, key, vector):
    table[key] = [p + q for p, q in zip(table[key], vector)] if key in table else list(vector)


def cell_gradients(offsets, flip_y, flip_z):
    offsets = swap_corners(offsets, flip_y, flip_z)
    sign_y, sign_z = jnp.where(flip_y, -1.0, 1.0), jnp.where(flip_z, -1.0, 1.0)
    anchor = offsets[0, 0, 0]
    edges = {}
    for vertex in CORNERS[1:]:
        edge = [p - q for p, q in zip(offsets[vertex], anchor)]
        if vertex[0]:
            edge[0] = edge[0] + 1.0
        if vertex[1]:
            edge[1] = edge[1] + sign_y
        if vertex[2]:
            edge[2] = edge[2] + sign_z
        edges[vertex] = edge
    gradients, diagonal = [], {}
    for path in paths():
        one, two, three = [edges[v] for v in path]
        across = [cross(two, three), cross(three, one), cross(one, two)]
        volume = one[0] * across[0][0] + one[1] * across[0][1] + one[2] * across[0][2]
        inverse = 1.0 / volume
        grads = [[p * inverse for p in vector] for vector in across]
        gradients.append(grads)
        first = [-(grads[0][p] + grads[1][p] + grads[2][p]) for p in range(3)]
        for vertex, grad in zip([(0, 0, 0)] + path, [first] + grads):
            square = [p * p for p in grad]
            norm = square[0] + square[1] + square[2]
            add_to(diagonal, vertex, [(LAMBDA_RATIO + 1.0) * p + norm for p in square])
    return gradients, swap_corners(diagonal, flip_y, flip_z)


def cell_forces(gradients, motion, flip_y, flip_z):
    motion = swap_corners(motion, flip_y, flip_z)
    anchor = motion[0, 0, 0]
    moves = {v: [p - q for p, q in zip(motion[v], anchor)] for v in CORNERS[1:]}
    forces = {}
    for tet, path in enumerate(paths()):
        grads = [[gradients(tet, v, p) for p in range(3)] for v in range(3)]
        tensor = [
            [
                moves[path[0]][p] * grads[0][q]
                + moves[path[1]][p] * grads[1][q]
                + moves[path[2]][p] * grads[2][q]
                for q in range(3)
            ]
            for p in range(3)
        ]
        trace = LAMBDA_RATIO * (tensor[0][0] + tensor[1][1] + tensor[2][2])
        stress = [[None] * 3 for _ in range(3)]
        for p in range(3):
            stress[p][p] = tensor[p][p] + tensor[p][p] + trace
            for q in range(p):
                stress[p][q] = stress[q][p] = tensor[p][q] + tensor[q][p]
        for v in range(3):
            add_to(
                forces,
                path[v],
                [
                    stress[p][0] * grads[v][0] + stress[p][1] * grads[v][1] + stress[p][2] * grads[v][2]
                    for p in range(3)
                ],
            )
    first = None
    for vector in forces.values():
        first = vector if first is None else [p + q for p, q in zip(first, vector)]
    forces[0, 0, 0] = [-p for p in first]
    return swap_corners(forces, flip_y, flip_z)


def turn(x, shift, axis):
    shift %= x.shape[axis]
    return pltpu.roll(x, shift, axis) if shift else x


def float_codes(value):
    return value >= 1.5, (value == 1.0) | (value == 3.0)


def corners_of(low, high):
    corners = {}
    for b, row in ((0, low), (1, high)):
        for a in (0, 1):
            far = [turn(p, -a, 1) for p in row]
            corners[a, b, 0] = far
            corners[a, b, 1] = [turn(p, -1, 0) for p in far]
    return corners


def assemble_row(parts, b):
    near = [p + turn(q, 1, 0) for p, q in zip(parts[0, b, 0], parts[0, b, 1])]
    far = [p + turn(q, 1, 0) for p, q in zip(parts[1, b, 0], parts[1, b, 1])]
    return [p + turn(q, 1, 1) for p, q in zip(near, far)]


def one_hot(mask):
    return mask.astype(F32).astype(BF16)


def place_nodes(devices, capacity, own_ref, place_ref):
    rows = own_ref.shape[0]
    own = own_ref[...]
    upper = iota((LANES, LANES), 0) < iota((LANES, LANES), 1)
    prefix = jnp.concatenate([one_hot(upper), jnp.ones((LANES, LANES), BF16)], axis=0)
    lower = one_hot(iota((rows, rows), 1) < iota((rows, rows), 0))
    chunk = min(devices, 8)

    def ranks(step, place):
        masks = [own == step * chunk + o for o in range(chunk)]
        named = [one_hot(mask) for mask in masks]
        above = jnp.dot(lower, jnp.concatenate(named, axis=1), preferred_element_type=F32).astype(BF16)
        left = [
            jnp.concatenate([named[o], above[:, o * LANES : (o + 1) * LANES]], axis=1) for o in range(chunk)
        ]
        rank = jnp.dot(jnp.concatenate(left, axis=0), prefix, preferred_element_type=F32)
        for o in range(chunk):
            base = ((step * chunk + o) * capacity) * 1.0
            place = jnp.where(masks[o], rank[o * rows : (o + 1) * rows] + base, place)
        return place

    place = jnp.zeros((rows, LANES), F32)
    if devices <= 4 * chunk:
        for step in range(devices // chunk):
            place = ranks(step, place)
    else:
        place = lax.fori_loop(0, devices // chunk, ranks, place)
    place_ref[...] = place.astype(jnp.int32)


def pack_nodes(first, last, place_ref, val_ref, acc_ref):
    wide = 2 * LANES
    groups = acc_ref.shape[0] // 3
    pair = 16
    group_id = iota((groups, LANES), 0)
    lane_id = iota((wide, LANES), 0)

    def spread(step, carry):
        columns, parts = [], [[] for _ in range(6)]
        for u in range(ROW_STEP):
            row = step * ROW_STEP + u
            at = place_ref[pl.ds(row, 1), :]
            hit = one_hot(group_id == at // wide)
            columns.append(one_hot(lane_id == at % wide))
            for c in range(3):
                value = val_ref[pl.ds(c, 1), pl.ds(pl.multiple_of(row * LANES, LANES), LANES)]
                value = jnp.broadcast_to(value, (pair, LANES))
                high = value.astype(BF16)
                low = (value - high.astype(F32)).astype(BF16)
                for n, part in ((c, high), (3 + c, low)):
                    parts[n].append(hit * jnp.concatenate([part] * (groups // pair), axis=0))
        left = jnp.concatenate([jnp.concatenate(part, axis=1) for part in parts], axis=0)
        right = jnp.concatenate(columns, axis=1)
        product = lax.dot_general(left, right, (((1,), (1,)), ((), ())), preferred_element_type=F32)
        acc_ref[...] += product[: 3 * groups] + product[3 * groups :]
        return carry

    lax.fori_loop(first, last, spread, 0)


def window_kernel(
    counts,
    shell,
    owner,
    slot,
    weight,
    prev,
    offset,
    split,
    out,
    v_shell,
    v_owner,
    v_slot,
    v_weight,
    v_prev,
    v_offset,
    v_split,
    place,
    acc,
    packed,
    received,
    both,
    v_wall,
    tiles,
    near_in,
    wall_in,
    back_in,
    main_field,
    main_motion,
    main_force,
    main_grad,
    main_diag,
    edge_field,
    edge_motion,
    edge_grad,
    edge_diag,
    local_sem,
    near_send,
    near_recv,
    pack_send,
    pack_recv,
    wall_send,
    wall_recv,
    back_send,
    back_recv,
):
    num_struct, num_fluid = counts
    devices = num_struct * num_fluid
    s, f = lax.axis_index("struct"), lax.axis_index("fluid")
    me = s * num_fluid + f
    stencil, count_y, count_z, wall = slot.shape
    free = prev.shape[3] - wall
    nodes = count_y * count_z
    deep = 2 * count_z
    span = count_y * COLUMNS
    pitch = LANES // count_y
    share = free // num_struct
    rows_own = v_owner.shape[0]
    capacity = 2 * rows_own * LANES // devices
    pieces = capacity // LANES
    groups = devices * pieces
    far_wall = 2 * SWEEPS + SWEEPS + 1

    def peer(ds, df):
        return ((s + ds + num_struct) % num_struct, (f + df + num_fluid) % num_fluid)

    def remote(src, dst, send, recv, where):
        return pltpu.make_async_remote_copy(
            src_ref=src, dst_ref=dst, send_sem=send, recv_sem=recv, device_id=where, device_id_type=MESH
        )

    loads = [
        (owner, v_owner),
        (offset, v_offset),
        (split, v_split),
        (prev.at[:, :, :, pl.ds(wall, free)], v_prev),
        (shell, v_shell),
        (slot, v_slot),
        (weight, v_weight),
    ]
    loads = [pltpu.make_async_copy(a, b, local_sem.at[n]) for n, (a, b) in enumerate(loads)]
    for load in loads:
        load.start()

    barrier = pltpu.get_barrier_semaphore()

    def greet(d, carry):
        other = (me + d) % devices
        pl.semaphore_signal(
            barrier, inc=1, device_id=(other // num_fluid, other % num_fluid), device_id_type=MESH
        )
        return carry

    lax.fori_loop(1, devices, greet, 0)

    with jax.named_scope("place"):
        loads[0].wait()
        place_nodes(devices, capacity, v_owner, place)

    lane = iota((count_z, LANES), 1)
    with jax.named_scope("tiles"):
        for load in loads[1:4]:
            load.wait()
        slab = jnp.zeros((count_z, LANES), F32)
        for n in range(7):
            shifted = [[None] * count_y for _ in range(num_struct)]
            for j in range(count_y):
                if n < 3:
                    near, far = v_offset[n, j, :, :wall], v_offset[n, j, :, wall:]
                elif n == 3:
                    near, far = v_split[j, :, :wall].astype(F32), v_split[j, :, wall:].astype(F32)
                else:
                    near, far = jnp.zeros((count_z, LANES), F32), v_prev[n - 4, j]
                for q in range(num_struct):
                    begin = share * q - SWEEPS
                    line = far
                    if begin < 0:
                        line = jnp.where(lane >= LANES + begin, near, far)
                    if begin + pitch > LANES:
                        line = jnp.where(lane < begin + pitch - LANES, near, far)
                    shifted[q][j] = turn(line, pitch * j - begin, 1)
                if n < 4:
                    base = span * n + COLUMNS * j
                    low = turn(jnp.where(lane == LANES - 1, near, far), base + 1, 1)
                    high = turn(jnp.where(lane == 0, near, far), base + far_wall, 1)
                    slab = jnp.where((lane >= base) & (lane < base + 2 * SWEEPS), low, slab)
                    slab = jnp.where(
                        (lane >= base + 2 * SWEEPS) & (lane < base + COLUMNS), high, slab
                    )
            for q in range(num_struct):
                total = shifted[q][0]
                for j in range(1, count_y):
                    total = jnp.where(lane >= pitch * j, shifted[q][j], total)
                tiles[q, n] = total
        for q in range(num_struct):
            tiles[q, 7] = slab

    with jax.named_scope("barrier"):
        pl.semaphore_wait(barrier, devices - 1)

    around = [(r, df) for r in range(num_struct) for df in (0, -1, 1) if (r, df) != (0, 0)]

    def planes_of(df):
        return pl.ds(0, count_z) if df == 0 else pl.ds(0 if df > 0 else SWEEPS, SWEEPS)

    def near_copy(r, df):
        to = peer(-r, -df)
        return remote(
            tiles.at[to[0], :, planes_of(df)],
            near_in.at[r, 0 if df == 0 else 1, :, planes_of(df)],
            near_send.at[r, df + 1],
            near_recv.at[r, df + 1],
            to,
        )

    near_copies = [near_copy(r, df) for r, df in around]
    for copy in near_copies:
        copy.start()
    near_in[0, 0] = tiles[s]

    with jax.named_scope("pack"):
        acc[...] = jnp.zeros_like(acc)
        loads[4].wait()
        pack_nodes(0, rows_own // ROW_STEP, place, v_shell, acc)
    with jax.named_scope("relay"):
        pack_groups = groups // 2
        for o in range(devices):
            for c in range(3):
                for b in range(pieces):
                    m = o * pieces + b
                    packed[o, pl.ds(c * pieces + b, 1), :] = acc[
                        pl.ds(c * pack_groups + m // 2, 1), pl.ds((m % 2) * LANES, LANES)
                    ]

    with jax.named_scope("sendpack"):

        def send_pack(d, carry):
            other = (me + d) % devices
            remote(
                packed.at[other],
                received.at[me],
                pack_send,
                pack_recv,
                (other // num_fluid, other % num_fluid),
            ).start()
            return carry

        lax.fori_loop(1, devices, send_pack, 0)
        received[me] = packed[me]
    all_packs = remote(
        packed.at[pl.ds(0, devices - 1)],
        received.at[pl.ds(0, devices - 1)],
        pack_send,
        pack_recv,
        peer(1, 0),
    )

    lane_deep = iota((deep, LANES), 1)
    row_low = lane_deep < pitch
    column = lane_deep % pitch + share * s
    free_node = (column >= SWEEPS) & (column < free + SWEEPS)

    def main_row(read, r):
        following = (r + 1) % num_struct
        low = [read(r, c) for c in range(3)]
        high = [
            jnp.where(row_low, turn(p, pitch, 1), turn(read(following, c), pitch, 1))
            for c, p in enumerate(low)
        ]
        return corners_of(low, high), following

    def main_add(ref, r, following, parts):
        for c, (low, high) in enumerate(zip(assemble_row(parts, 0), assemble_row(parts, 1))):
            moved = turn(high, pitch, 1)
            ref[r, c] = ref[r, c] + low + jnp.where(row_low, 0.0, moved)
            ref[following, c] = ref[following, c] + jnp.where(row_low, moved, 0.0)

    def prepare_main():
        main_diag[...] = jnp.zeros_like(main_diag)
        for r in range(num_struct):
            for n in range(FIELDS):
                whole = jnp.concatenate([near_in[r, 0, n], near_in[r, 1, n]], axis=0)
                if n < 4:
                    main_field[r, n] = whole
                elif n < 7:
                    main_motion[r, n - 4] = whole
                else:
                    for m in range(4):
                        moved = turn(whole, span * (r - m), 1)
                        if r == 0:
                            edge_field[m] = moved
                        else:
                            edge_field[m] = jnp.where(lane_deep >= span * r, moved, edge_field[m])

        def row(r, carry):
            corners, following = main_row(lambda at, c: main_field[at, c], r)
            gradients, parts = cell_gradients(corners, *float_codes(main_field[r, 3]))
            for tet in range(6):
                for v in range(3):
                    for p in range(3):
                        main_grad[r, 9 * tet + 3 * v + p] = gradients[tet][v][p]
            main_add(main_diag, r, following, parts)
            return carry

        lax.fori_loop(0, num_struct, row, 0)

    def sweep_main(sweep, carry):
        main_force[...] = jnp.zeros_like(main_force)

        def row(r, inner):
            corners, following = main_row(lambda at, c: main_motion[at, c], r)
            parts = cell_forces(
                lambda tet, v, p: main_grad[r, 9 * tet + 3 * v + p],
                corners,
                *float_codes(main_field[r, 3]),
            )
            main_add(main_force, r, following, parts)
            return inner

        lax.fori_loop(0, num_struct, row, 0)
        for r in range(num_struct):
            for c in range(3):
                now = main_motion[r, c]
                change = RELAX_FACTOR * main_force[r, c] / main_diag[r, c]
                main_motion[r, c] = jnp.where(free_node, now - change, now)
        return carry

    def edge_corners(values):
        return corners_of(values, [turn(p, -COLUMNS, 1) for p in values])

    def edge_assemble(parts):
        low, high = assemble_row(parts, 0), assemble_row(parts, 1)
        return [p + turn(q, COLUMNS, 1) for p, q in zip(low, high)]

    def prepare_edge():
        gradients, parts = cell_gradients(
            edge_corners([edge_field[c] for c in range(3)]), *float_codes(edge_field[3])
        )
        for tet in range(6):
            for v in range(3):
                for p in range(3):
                    edge_grad[9 * tet + 3 * v + p] = gradients[tet][v][p]
        for c, value in enumerate(edge_assemble(parts)):
            edge_diag[c] = value

    def plane_points(ref, zero):
        row, at = iota((nodes, LANES), 0), iota((nodes, LANES), 1)
        within = row // count_z * (2 * count_z) + count_z - 1 - row % count_z
        total = None
        for t in range(stencil):
            whole = jnp.concatenate([ref[t, j] for j in range(count_y)], axis=0)
            for side in (0, 1):
                edge = wall - 1 if side == 0 else 0
                spread = jnp.broadcast_to(whole[:, edge : edge + 1], (nodes, LANES))
                part = jnp.where(at == 2 * nodes * t + count_z * side + within, spread, zero)
                total = part if total is None else total + part
        return jnp.sum(total, axis=0, keepdims=True)

    with jax.named_scope("waitnear"):
        for copy in near_copies:
            copy.wait_recv()
    with jax.named_scope("prepmain"):
        prepare_main()
    with jax.named_scope("sweeps"):
        lax.fori_loop(0, SWEEPS, sweep_main, 0)

    def back_copy(r):
        at = (s + r) % num_struct
        return remote(
            main_motion.at[r, :, pl.ds(0, count_z)],
            back_in.at[s],
            back_send.at[r],
            back_recv.at[s],
            peer(r, 0),
        ), remote(
            main_motion.at[r, :, pl.ds(0, count_z)],
            back_in.at[at],
            back_send.at[r],
            back_recv.at[at],
            peer(r, 0),
        )

    back_copies = [back_copy(r) for r in range(1, num_struct)]
    for copy, _ in back_copies:
        copy.start()
    back_in[s] = main_motion[0, :, :count_z, :]
    with jax.named_scope("prepedge"):
        prepare_edge()
    with jax.named_scope("points"):
        loads[5].wait()
        loads[6].wait()
        plane_slot, plane_weight = plane_points(v_slot, 0), plane_points(v_weight, 0.0)

    with jax.named_scope("waitpack"):
        all_packs.wait_recv()

    with jax.named_scope("table"):
        for c in range(3):
            whole = jnp.concatenate(
                [received[o, pl.ds(c * pieces, pieces), :] for o in range(devices)], axis=0
            )
            high, low = split_two(whole)
            both[pl.ds(c * groups, groups), :LANES] = high
            both[pl.ds(c * groups, groups), LANES:] = low

    with jax.named_scope("planes"):
        pick = one_hot(iota((LANES, LANES), 0) == plane_slot % LANES)
        found = jnp.dot(both[...], jnp.concatenate([pick, pick], axis=0), preferred_element_type=F32)
        scaled = jnp.where(iota((groups, LANES), 0) == plane_slot // LANES, plane_weight, 0.0)
        tile = jnp.zeros((count_z, LANES), F32)
        for c in range(3):
            line = jnp.sum(found[c * groups : (c + 1) * groups] * scaled, axis=0, keepdims=True)
            period = LANES // 2
            while period >= 2 * nodes:
                line = line + turn(line, period, 1)
                period //= 2
            spread = pltpu.roll(jnp.broadcast_to(line, (count_z, LANES)), 0, 1, stride=1, stride_axis=0)
            tile = jnp.where((lane >= span * c) & (lane < span * (c + 1)), spread, tile)
        wall_in[0, 0] = tile

    def wall_copy(r, df):
        return remote(
            wall_in.at[0, 0, planes_of(df)],
            wall_in.at[r, 0 if df == 0 else 1, planes_of(df)],
            wall_send.at[r, df + 1],
            wall_recv.at[r, df + 1],
            peer(-r, -df),
        )

    wall_copies = [wall_copy(r, df) for r, df in around]
    for copy in wall_copies:
        copy.start()

    wide = 2 * LANES
    lane_id = iota((LANES, wide), 0)
    group_id = iota((groups, wide), 0)

    def pair(step, carry):
        j, k = 2 * step // count_z, 2 * step % count_z
        sums = [None] * 3
        for t in range(stencil):
            at = jnp.concatenate(
                [v_slot[t, j, pl.ds(k, 1), :], v_slot[t, j, pl.ds(k + 1, 1), :]], axis=1
            )
            by = jnp.concatenate(
                [v_weight[t, j, pl.ds(k, 1), :], v_weight[t, j, pl.ds(k + 1, 1), :]], axis=1
            )
            choose = one_hot(lane_id == at % LANES)
            values = jnp.dot(
                both[...], jnp.concatenate([choose, choose], axis=0), preferred_element_type=F32
            )
            factor = jnp.where(group_id == at // LANES, by, 0.0)
            for c in range(3):
                term = values[c * groups : (c + 1) * groups] * factor
                sums[c] = term if sums[c] is None else sums[c] + term
        for c in range(3):
            line = jnp.sum(sums[c], axis=0, keepdims=True)
            v_wall[c, pl.ds(2 * step, 1), :] = line[:, :LANES]
            v_wall[c, pl.ds(2 * step + 1, 1), :] = line[:, LANES:]
        return carry

    with jax.named_scope("wall"):
        lax.fori_loop(0, nodes // 2, pair, 0)

    with jax.named_scope("waitwall"):
        for copy in wall_copies:
            copy.wait_recv()
    with jax.named_scope("edgeinit"):
        within = lane_deep % COLUMNS
        inner = ((within >= 1) & (within <= SWEEPS)) | ((within > 2 * SWEEPS) & (within < far_wall))
        arrived = [jnp.concatenate([wall_in[r, 0], wall_in[r, 1]], axis=0) for r in range(num_struct)]
        for c in range(3):
            total = jnp.zeros((deep, LANES), F32)
            for r in range(num_struct):
                here = lane_deep // span == r
                shift = span * (r - c) - (count_z - 1)
                total = jnp.where(here & (within == 0), turn(arrived[r], shift, 1), total)
                shift = shift - count_z + far_wall
                total = jnp.where(here & (within == far_wall), turn(arrived[r], shift, 1), total)
            edge_motion[c] = total

    def sweep_edge(step, carry):
        parts = cell_forces(
            lambda tet, v, p: edge_grad[9 * tet + 3 * v + p],
            edge_corners([edge_motion[c] for c in range(3)]),
            *float_codes(edge_field[3]),
        )
        for c, value in enumerate(edge_assemble(parts)):
            now = edge_motion[c]
            edge_motion[c] = jnp.where(inner, now - RELAX_FACTOR * value / edge_diag[c], now)
        return carry

    with jax.named_scope("sweepedge"):
        lax.fori_loop(0, SWEEPS, sweep_edge, 0)

    with jax.named_scope("waitback"):
        for _, copy in back_copies:
            copy.wait_recv()
    with jax.named_scope("outs"):
        for c in range(3):
            for j in range(count_y):
                out[c, j, :, :wall] = v_wall[c, pl.ds(j * count_z, count_z), :]
                total = None
                for q in range(num_struct):
                    moved = turn(back_in[q, c], share * q - pitch * j - SWEEPS, 1)
                    total = moved if total is None else jnp.where(lane >= share * q, moved, total)
                delta = edge_motion[c, :count_z, :]
                low = turn(delta, -1 - COLUMNS * j, 1)
                high = turn(delta, free - far_wall - COLUMNS * j, 1)
                change = jnp.where(lane < SWEEPS, low, jnp.where(lane >= free - SWEEPS, high, 0.0))
                out[c, j, :, wall:] = total + change

    with jax.named_scope("waitsend"):
        for copy in near_copies + wall_copies + [copy for copy, _ in back_copies]:
            copy.wait_send()
        all_packs.wait_send()


def shards(shell_motion, owner, stencil_slot, stencil_weight, prev_motion, node_offset, cell_split):
    num_struct, num_fluid = lax.axis_size("struct"), lax.axis_size("fluid")
    devices = num_struct * num_fluid
    own = shell_motion.shape[1]
    pieces = 2 * own // devices // LANES
    groups = devices * pieces
    stencil, count_y, count_z, wall = stencil_slot.shape
    total_x = prev_motion.shape[3]
    free = total_x - wall
    nodes, deep = count_y * count_z, 2 * count_z
    assert wall == free == LANES and count_z == 2 * SWEEPS == 8 and num_struct >= 2 and num_fluid >= 3
    assert num_struct * count_y * COLUMNS == LANES and 2 * stencil * nodes == LANES
    assert free // num_struct + 2 * SWEEPS <= LANES // count_y
    vmem, dma = pltpu.VMEM, pltpu.SemaphoreType.DMA
    scratch = [
        vmem((3, own), F32),
        vmem((own // LANES, LANES), jnp.int32),
        vmem((stencil, count_y, count_z, wall), jnp.int32),
        vmem((stencil, count_y, count_z, wall), F32),
        vmem((3, count_y, count_z, free), F32),
        vmem((3, count_y, count_z, total_x), F32),
        vmem((count_y, count_z, total_x), jnp.int32),
        vmem((own // LANES, LANES), jnp.int32),
        vmem((3 * groups // 2, 2 * LANES), F32),
        vmem((devices, 3 * pieces, LANES), F32),
        vmem((devices, 3 * pieces, LANES), F32),
        vmem((3 * groups, 2 * LANES), BF16),
        vmem((3, nodes, wall), F32),
        vmem((num_struct, FIELDS, count_z, LANES), F32),
        vmem((num_struct, 2, FIELDS, count_z, LANES), F32),
        vmem((num_struct, 2, count_z, LANES), F32),
        vmem((num_struct, 3, count_z, LANES), F32),
        vmem((num_struct, 4, deep, LANES), F32),
        vmem((num_struct, 3, deep, LANES), F32),
        vmem((num_struct, 3, deep, LANES), F32),
        vmem((num_struct, 54, deep, LANES), F32),
        vmem((num_struct, 3, deep, LANES), F32),
        vmem((4, deep, LANES), F32),
        vmem((3, deep, LANES), F32),
        vmem((54, deep, LANES), F32),
        vmem((3, deep, LANES), F32),
        dma((7,)),
        dma((num_struct, 3)),
        dma((num_struct, 3)),
        dma,
        dma,
        dma((num_struct, 3)),
        dma((num_struct, 3)),
        dma((num_struct,)),
        dma((num_struct,)),
    ]
    return pl.pallas_call(
        functools.partial(window_kernel, (num_struct, num_fluid)),
        out_shape=pltpu.VMEM(prev_motion.shape, F32),
        in_specs=[pl.BlockSpec(memory_space=pltpu.HBM)] * 7,
        out_specs=pl.BlockSpec(memory_space=pltpu.VMEM),
        scratch_shapes=scratch,
        cost_estimate=pl.CostEstimate(flops=4 << 30, bytes_accessed=16 << 20, transcendentals=0),
        compiler_params=pltpu.CompilerParams(
            collective_id=0, has_side_effects=True, vmem_limit_bytes=67043328 - (1 << 17)
        ),
    )(
        shell_motion,
        owner.reshape(own // LANES, LANES),
        stencil_slot,
        stencil_weight,
        prev_motion,
        node_offset,
        cell_split,
    )


def solution(mesh):
    return jax.shard_map(
        shards,
        mesh=mesh,
        in_specs=(
            P(None, ("struct", "fluid")),
            P(("struct", "fluid"), None),
            P(None, "struct", "fluid", None),
            P(None, "struct", "fluid", None),
            P(None, "struct", "fluid", None),
            P(None, "struct", "fluid", None),
            P("struct", "fluid", None),
        ),
        out_specs=P(None, "struct", "fluid", None),
        check_vma=False,
    )
```

```python
import functools

import jax
import jax.numpy as jnp
from jax import lax
from jax.experimental import pallas as pl
from jax.experimental.pallas import tpu as pltpu
from jax.sharding import PartitionSpec as P

SWEEPS = 4
LANES = 128
LAMBDA_RATIO = 1.0
RELAX_FACTOR = 0.5
STEP_ORDERS = ((0, 1, 2), (0, 2, 1), (1, 0, 2), (1, 2, 0), (2, 0, 1), (2, 1, 0))
CORNERS = tuple((a, b, c) for a in (0, 1) for b in (0, 1) for c in (0, 1))
COLUMNS = 16
FIELDS = 8
ROW_STEP = 16
WALL_STEP = 4
EARLY_SWEEPS = 2
MESH = pl.DeviceIdType.MESH
BF16 = jnp.bfloat16
F32 = jnp.float32


def split_two(values):
    high = values.astype(BF16)
    low = (values - high.astype(F32)).astype(BF16)
    return high, low


def iota(shape, dim):
    return lax.broadcasted_iota(jnp.int32, shape, dim)


def swap_corners(corners, flip_y, flip_z):
    middle = {}
    for a, b, c in CORNERS:
        middle[a, b, c] = [
            jnp.where(flip_y, q, p) for p, q in zip(corners[a, b, c], corners[a, 1 - b, c])
        ]
    return {
        (a, b, c): [jnp.where(flip_z, q, p) for p, q in zip(middle[a, b, c], middle[a, b, 1 - c])]
        for a, b, c in CORNERS
    }


def paths():
    for order in STEP_ORDERS:
        position, path = [0, 0, 0], []
        for axis_id in order:
            position[axis_id] = 1
            path.append(tuple(position))
        yield path


def cross(p, q):
    return [p[1] * q[2] - p[2] * q[1], p[2] * q[0] - p[0] * q[2], p[0] * q[1] - p[1] * q[0]]


def add_to(table, key, vector):
    table[key] = [p + q for p, q in zip(table[key], vector)] if key in table else list(vector)


RING = ((1, 0, 0), (1, 1, 0), (0, 1, 0), (0, 1, 1), (0, 0, 1), (1, 0, 1))
TOP = (1, 1, 1)


def ring_tets():
    order = [tuple(path) for path in paths()]
    for k in range(6):
        one, two = RING[k], RING[(k + 1) % 6]
        if sum(one) > sum(two):
            one, two = two, one
        yield order.index((one, two, TOP)), (one, two, TOP)


def slot_of(corner, p):
    return 3 * CORNERS.index(corner) + p


def halves(ref):
    rows = ref.shape[1]
    return [pl.ds(h, 8) for h in range(0, rows, 8)]


def finish(sums, k, give):
    done = []
    if k > 0:
        done.append(RING[k])
    if k == 5:
        done += [RING[0], TOP]
    for corner in done:
        give(corner, sums.pop(corner))


def open_gradients(offsets, flips, work):
    offsets = swap_corners(offsets, *flips)
    signs = [None] + [jnp.where(flip, -1.0, 1.0) for flip in flips]
    anchor = offsets[0, 0, 0]
    for vertex in CORNERS[1:]:
        for p in range(3):
            edge = offsets[vertex][p] - anchor[p]
            if vertex[p]:
                edge = edge + (signs[p] if p else 1.0)
            work[0, slot_of(vertex, p)] = edge


def fill_gradients(work, put):
    for rows in halves(work.at[0]):
        sums = {}
        for k, (tet, path) in enumerate(ring_tets()):
            one, two, three = [[work[0, slot_of(v, p), rows] for p in range(3)] for v in path]
            across = [cross(two, three), cross(three, one), cross(one, two)]
            inverse = 1.0 / (one[0] * across[0][0] + one[1] * across[0][1] + one[2] * across[0][2])
            grads = [[p * inverse for p in vector] for vector in across]
            for v in range(3):
                for p in range(3):
                    put(9 * tet + 3 * v + p, rows, grads[v][p])
            first = [grads[0][p] + grads[1][p] + grads[2][p] for p in range(3)]
            for vertex, grad in zip(((0, 0, 0),) + path, [first] + grads):
                square = [p * p for p in grad]
                norm = square[0] + square[1] + square[2]
                add_to(sums, vertex, [(LAMBDA_RATIO + 1.0) * p + norm for p in square])

            def give(corner, vector):
                for p in range(3):
                    work[1, slot_of(corner, p), rows] = vector[p]

            finish(sums, k, give)
        give((0, 0, 0), sums[0, 0, 0])


def close_cells(work, flips):
    parts = swap_corners({v: [work[1, slot_of(v, p)] for p in range(3)] for v in CORNERS}, *flips)
    return {
        (a, b): [p + turn(q, 1, 0) for p, q in zip(parts[a, b, 0], parts[a, b, 1])]
        for a in (0, 1)
        for b in (0, 1)
    }


def open_forces(motion, flips, work):
    motion = swap_corners(motion, *flips)
    anchor = motion[0, 0, 0]
    for vertex in CORNERS[1:]:
        for p in range(3):
            work[0, slot_of(vertex, p)] = motion[vertex][p] - anchor[p]


def fill_forces(get, work):
    for rows in halves(work.at[0]):
        sums, total = {}, [None]
        top = [work[0, slot_of(TOP, p), rows] for p in range(3)]
        for k, (tet, path) in enumerate(ring_tets()):
            grads = [[get(9 * tet + 3 * v + p, rows) for p in range(3)] for v in range(3)]
            moves = [[work[0, slot_of(v, p), rows] for p in range(3)] for v in path[:2]] + [top]
            tensor = [
                [
                    moves[0][p] * grads[0][q] + moves[1][p] * grads[1][q] + moves[2][p] * grads[2][q]
                    for q in range(3)
                ]
                for p in range(3)
            ]
            trace = LAMBDA_RATIO * (tensor[0][0] + tensor[1][1] + tensor[2][2])
            stress = [[None] * 3 for _ in range(3)]
            for p in range(3):
                stress[p][p] = tensor[p][p] + tensor[p][p] + trace
                for q in range(p):
                    stress[p][q] = stress[q][p] = tensor[p][q] + tensor[q][p]
            for v in range(3):
                add_to(
                    sums,
                    path[v],
                    [
                        stress[p][0] * grads[v][0] + stress[p][1] * grads[v][1] + stress[p][2] * grads[v][2]
                        for p in range(3)
                    ],
                )

            def give(corner, vector):
                for p in range(3):
                    work[1, slot_of(corner, p), rows] = vector[p]
                total[0] = vector if total[0] is None else [p + q for p, q in zip(total[0], vector)]

            finish(sums, k, give)
        for p in range(3):
            work[1, p, rows] = -total[0][p]


def turn(x, shift, axis):
    shift %= x.shape[axis]
    return pltpu.roll(x, shift, axis) if shift else x


def float_codes(value):
    return value >= 1.5, (value == 1.0) | (value == 3.0)


def with_planes(edges):
    corners = {}
    for (a, b), values in edges.items():
        corners[a, b, 0] = values
        corners[a, b, 1] = [turn(p, -1, 0) for p in values]
    return corners


def one_hot(mask):
    return mask.astype(F32).astype(BF16)


def place_nodes(devices, capacity, own_ref, place_ref):
    rows = own_ref.shape[0]
    own = own_ref[...]
    upper = iota((LANES, LANES), 0) < iota((LANES, LANES), 1)
    prefix = jnp.concatenate([one_hot(upper), jnp.ones((LANES, LANES), BF16)], axis=0)
    lower = one_hot(iota((rows, rows), 1) < iota((rows, rows), 0))
    chunk = min(devices, 8)

    def ranks(step, place):
        masks = [own == step * chunk + o for o in range(chunk)]
        named = [one_hot(mask) for mask in masks]
        above = jnp.dot(lower, jnp.concatenate(named, axis=1), preferred_element_type=F32).astype(BF16)
        left = [
            jnp.concatenate([named[o], above[:, o * LANES : (o + 1) * LANES]], axis=1) for o in range(chunk)
        ]
        rank = jnp.dot(jnp.concatenate(left, axis=0), prefix, preferred_element_type=F32)
        for o in range(chunk):
            base = ((step * chunk + o) * capacity) * 1.0
            place = jnp.where(masks[o], rank[o * rows : (o + 1) * rows] + base, place)
        return place

    place = jnp.zeros((rows, LANES), F32)
    if devices <= 4 * chunk:
        for step in range(devices // chunk):
            place = ranks(step, place)
    else:
        place = lax.fori_loop(0, devices // chunk, ranks, place)
    place_ref[...] = place.astype(jnp.int32)


def pack_nodes(first, last, place_ref, val_ref, acc_ref):
    wide = 2 * LANES
    groups = acc_ref.shape[0] // 3
    pair = 16
    group_id = iota((groups, LANES), 0)
    lane_id = iota((wide, LANES), 0)

    def spread(step, carry):
        columns, parts = [], [[] for _ in range(6)]
        for u in range(ROW_STEP):
            row = step * ROW_STEP + u
            at = place_ref[pl.ds(row, 1), :]
            hit = one_hot(group_id == at // wide)
            columns.append(one_hot(lane_id == at % wide))
            for c in range(3):
                value = val_ref[pl.ds(c, 1), pl.ds(pl.multiple_of(row * LANES, LANES), LANES)]
                value = jnp.broadcast_to(value, (pair, LANES))
                high = value.astype(BF16)
                low = (value - high.astype(F32)).astype(BF16)
                for n, part in ((c, high), (3 + c, low)):
                    parts[n].append(hit * jnp.concatenate([part] * (groups // pair), axis=0))
        left = jnp.concatenate([jnp.concatenate(part, axis=1) for part in parts], axis=0)
        right = jnp.concatenate(columns, axis=1)
        product = lax.dot_general(left, right, (((1,), (1,)), ((), ())), preferred_element_type=F32)
        acc_ref[...] += product[: 3 * groups] + product[3 * groups :]
        return carry

    lax.fori_loop(first, last, spread, 0)


def window_kernel(
    counts,
    shell,
    owner,
    slot,
    weight,
    prev,
    offset,
    split,
    out,
    v_shell,
    v_owner,
    v_slot,
    v_weight,
    v_prev,
    v_offset,
    v_split,
    place,
    acc,
    packed,
    received,
    both,
    v_wall,
    tiles,
    near_in,
    wall_in,
    back_in,
    main_field,
    main_motion,
    main_grad,
    main_scale,
    edge_field,
    edge_motion,
    edge_grad,
    edge_scale,
    work,
    local_sem,
    near_send,
    near_recv,
    pack_send,
    pack_recv,
    wall_send,
    wall_recv,
    back_send,
    back_recv,
):
    num_struct, num_fluid = counts
    devices = num_struct * num_fluid
    s, f = lax.axis_index("struct"), lax.axis_index("fluid")
    me = s * num_fluid + f
    stencil, count_y, count_z, wall = slot.shape
    free = prev.shape[3] - wall
    nodes = count_y * count_z
    deep = 2 * count_z
    span = count_y * COLUMNS
    pitch = LANES // count_y
    share = free // num_struct
    rows_own = v_owner.shape[0]
    capacity = 2 * rows_own * LANES // devices
    pieces = capacity // LANES
    groups = devices * pieces
    far_wall = 2 * SWEEPS + SWEEPS + 1

    def peer(ds, df):
        return ((s + ds + num_struct) % num_struct, (f + df + num_fluid) % num_fluid)

    def remote(src, dst, send, recv, where):
        return pltpu.make_async_remote_copy(
            src_ref=src, dst_ref=dst, send_sem=send, recv_sem=recv, device_id=where, device_id_type=MESH
        )

    loads = [
        (owner, v_owner),
        (offset, v_offset),
        (split, v_split),
        (prev.at[:, :, :, pl.ds(wall, free)], v_prev),
        (shell, v_shell),
        (slot, v_slot),
        (weight, v_weight),
    ]
    loads = [pltpu.make_async_copy(a, b, local_sem.at[n]) for n, (a, b) in enumerate(loads)]
    for load in loads:
        load.start()

    barrier = pltpu.get_barrier_semaphore()

    def greet(d, carry):
        other = (me + d) % devices
        pl.semaphore_signal(
            barrier, inc=1, device_id=(other // num_fluid, other % num_fluid), device_id_type=MESH
        )
        return carry

    lax.fori_loop(1, devices, greet, 0)

    with jax.named_scope("place"):
        loads[0].wait()
        place_nodes(devices, capacity, v_owner, place)

    lane = iota((count_z, LANES), 1)
    with jax.named_scope("tiles"):
        for load in loads[1:4]:
            load.wait()
        slab = jnp.zeros((count_z, LANES), F32)
        for n in range(7):
            shifted = [[None] * count_y for _ in range(num_struct)]
            for j in range(count_y):
                if n < 3:
                    near, far = v_offset[n, j, :, :wall], v_offset[n, j, :, wall:]
                elif n == 3:
                    near, far = v_split[j, :, :wall].astype(F32), v_split[j, :, wall:].astype(F32)
                else:
                    near, far = jnp.zeros((count_z, LANES), F32), v_prev[n - 4, j]
                for q in range(num_struct):
                    begin = share * q - SWEEPS
                    line = far
                    if begin < 0:
                        line = jnp.where(lane >= LANES + begin, near, far)
                    if begin + pitch > LANES:
                        line = jnp.where(lane < begin + pitch - LANES, near, far)
                    shifted[q][j] = turn(line, pitch * j - begin, 1)
                if n < 4:
                    base = span * n + COLUMNS * j
                    low = turn(jnp.where(lane == LANES - 1, near, far), base + 1, 1)
                    high = turn(jnp.where(lane == 0, near, far), base + far_wall, 1)
                    slab = jnp.where((lane >= base) & (lane < base + 2 * SWEEPS), low, slab)
                    slab = jnp.where(
                        (lane >= base + 2 * SWEEPS) & (lane < base + COLUMNS), high, slab
                    )
            for q in range(num_struct):
                total = shifted[q][0]
                for j in range(1, count_y):
                    total = jnp.where(lane >= pitch * j, shifted[q][j], total)
                tiles[q, n] = total
        for q in range(num_struct):
            tiles[q, 7] = slab

    with jax.named_scope("barrier"):
        pl.semaphore_wait(barrier, devices - 1)

    around = [(r, df) for r in range(num_struct) for df in (0, -1, 1) if (r, df) != (0, 0)]

    def planes_of(df):
        return pl.ds(0, count_z) if df == 0 else pl.ds(0 if df > 0 else SWEEPS, SWEEPS)

    def near_copy(r, df):
        to = peer(-r, -df)
        return remote(
            tiles.at[to[0], :, planes_of(df)],
            near_in.at[2 * r + (df != 0), :, planes_of(df)],
            near_send,
            near_recv,
            to,
        )

    for r, df in around:
        near_copy(r, df).start()
    others = pl.ds(1, 2 * num_struct - 1)
    all_near = remote(near_in.at[others], near_in.at[others], near_send, near_recv, peer(1, 0))
    near_in[0] = tiles[s]

    with jax.named_scope("pack"):
        acc[...] = jnp.zeros_like(acc)
        loads[4].wait()
        pack_nodes(0, rows_own // ROW_STEP, place, v_shell, acc)
    with jax.named_scope("relay"):
        pack_groups = groups // 2
        for o in range(devices):
            for c in range(3):
                for b in range(pieces):
                    m = o * pieces + b
                    packed[o, pl.ds(c * pieces + b, 1), :] = acc[
                        pl.ds(c * pack_groups + m // 2, 1), pl.ds((m % 2) * LANES, LANES)
                    ]

    with jax.named_scope("sendpack"):

        def send_pack(d, carry):
            other = (me + d) % devices
            remote(
                packed.at[other],
                received.at[me],
                pack_send,
                pack_recv,
                (other // num_fluid, other % num_fluid),
            ).start()
            return carry

        lax.fori_loop(1, devices, send_pack, 0)
        received[me] = packed[me]
    all_packs = remote(
        packed.at[pl.ds(0, devices - 1)],
        received.at[pl.ds(0, devices - 1)],
        pack_send,
        pack_recv,
        peer(1, 0),
    )

    lane_deep = iota((deep, LANES), 1)
    row_low = lane_deep < pitch
    column = lane_deep % pitch + share * s
    within = lane_deep % COLUMNS
    inner = ((within >= 1) & (within <= SWEEPS)) | ((within > 2 * SWEEPS) & (within < far_wall))
    free_node = (column >= SWEEPS) & (column < free + SWEEPS)

    def main_corners(read):
        values = [[read(r, c) for c in range(3)] for r in range(num_struct)]
        moved = [[[turn(p, n, 1) for p in row] for row in values] for n in (-1, pitch, pitch - 1)]
        for r in range(num_struct):
            high = [
                [jnp.where(row_low, p, q) for p, q in zip(moved[n][r], moved[n][(r + 1) % num_struct])]
                for n in (1, 2)
            ]
            yield r, with_planes(
                {(0, 0): values[r], (1, 0): moved[0][r], (0, 1): high[0], (1, 1): high[1]}
            )

    def main_sums():
        lows, highs = [], []
        for r in range(num_struct):
            ends = close_cells(work.at[r], float_codes(main_field[r, 3]))
            lows.append([p + turn(q, 1, 1) for p, q in zip(ends[0, 0], ends[1, 0])])
            highs.append(
                [turn(p, pitch, 1) + turn(q, pitch + 1, 1) for p, q in zip(ends[0, 1], ends[1, 1])]
            )
        for r in range(num_struct):
            yield r, [
                p + jnp.where(row_low, before, now) for p, before, now in zip(lows[r], highs[r - 1], highs[r])
            ]

    def prepare_main():
        for r in range(num_struct):
            for n in range(FIELDS):
                whole = jnp.concatenate([near_in[2 * r, n], near_in[2 * r + 1, n]], axis=0)
                if n < 4:
                    main_field[r, n] = whole
                elif n < 7:
                    main_motion[r, n - 4] = whole
                else:
                    for m in range(4):
                        moved = turn(whole, span * (r - m), 1)
                        if r == 0:
                            edge_field[m] = moved
                        else:
                            edge_field[m] = jnp.where(lane_deep >= span * r, moved, edge_field[m])

        for r, corners in main_corners(lambda at, c: main_field[at, c]):
            open_gradients(corners, float_codes(main_field[r, 3]), work.at[r])

        def row(r, carry):
            def put(n, rows, value):
                main_grad[r, n, rows] = value

            fill_gradients(work.at[r], put)
            return carry

        lax.fori_loop(0, num_struct, row, 0)
        for r, values in main_sums():
            for c in range(3):
                main_scale[r, c] = jnp.where(free_node, RELAX_FACTOR / values[c], 0.0)

    def sweep_main(sweep, carry):
        for r, corners in main_corners(lambda at, c: main_motion[at, c]):
            open_forces(corners, float_codes(main_field[r, 3]), work.at[r])

        for r in range(num_struct):
            fill_forces(lambda n, rows: main_grad[r, n, rows], work.at[r])
        for r, values in main_sums():
            for c in range(3):
                main_motion[r, c] = main_motion[r, c] - main_scale[r, c] * values[c]
        return carry

    def edge_corners(read):
        values = [read(c) for c in range(3)]
        return with_planes(
            {(a, b): [turn(p, -a - COLUMNS * b, 1) for p in values] for a in (0, 1) for b in (0, 1)}
        )

    def edge_sums():
        ends = close_cells(work.at[0], float_codes(edge_field[3]))
        moved = [[turn(p, a + COLUMNS * b, 1) for p in ends[a, b]] for a in (0, 1) for b in (0, 1)]
        return [(p + q) + (u + v) for p, q, u, v in zip(*moved)]

    def prepare_edge():
        open_gradients(edge_corners(lambda c: edge_field[c]), float_codes(edge_field[3]), work.at[0])

        def put(n, rows, value):
            edge_grad[n, rows] = value

        fill_gradients(work.at[0], put)
        for c, value in enumerate(edge_sums()):
            edge_scale[c] = jnp.where(inner, RELAX_FACTOR / value, 0.0)

    def plane_points(ref, zero):
        row, at = iota((nodes, LANES), 0), iota((nodes, LANES), 1)
        within = row // count_z * (2 * count_z) + count_z - 1 - row % count_z
        total = None
        for t in range(stencil):
            whole = jnp.concatenate([ref[t, j] for j in range(count_y)], axis=0)
            for side in (0, 1):
                edge = wall - 1 if side == 0 else 0
                spread = jnp.broadcast_to(whole[:, edge : edge + 1], (nodes, LANES))
                part = jnp.where(at == 2 * nodes * t + count_z * side + within, spread, zero)
                total = part if total is None else total + part
        return jnp.sum(total, axis=0, keepdims=True)

    with jax.named_scope("waitnear"):
        all_near.wait_recv()
    with jax.named_scope("prepmain"):
        prepare_main()
    with jax.named_scope("sweeps"):
        lax.fori_loop(0, EARLY_SWEEPS, sweep_main, 0)
    with jax.named_scope("prepedge"):
        prepare_edge()
    with jax.named_scope("points"):
        loads[5].wait()
        loads[6].wait()
        plane_slot, plane_weight = plane_points(v_slot, 0), plane_points(v_weight, 0.0)

    with jax.named_scope("waitpack"):
        all_packs.wait_recv()

    with jax.named_scope("table"):
        for c in range(3):
            whole = jnp.concatenate(
                [received[o, pl.ds(c * pieces, pieces), :] for o in range(devices)], axis=0
            )
            high, low = split_two(whole)
            both[pl.ds(c * groups, groups), :LANES] = high
            both[pl.ds(c * groups, groups), LANES:] = low

    with jax.named_scope("planes"):
        pick = one_hot(iota((LANES, LANES), 0) == plane_slot % LANES)
        found = jnp.dot(both[...], jnp.concatenate([pick, pick], axis=0), preferred_element_type=F32)
        scaled = jnp.where(iota((groups, LANES), 0) == plane_slot // LANES, plane_weight, 0.0)
        tile = jnp.zeros((count_z, LANES), F32)
        for c in range(3):
            line = jnp.sum(found[c * groups : (c + 1) * groups] * scaled, axis=0, keepdims=True)
            period = LANES // 2
            while period >= 2 * nodes:
                line = line + turn(line, period, 1)
                period //= 2
            spread = pltpu.roll(jnp.broadcast_to(line, (count_z, LANES)), 0, 1, stride=1, stride_axis=0)
            tile = jnp.where((lane >= span * c) & (lane < span * (c + 1)), spread, tile)
        wall_in[0] = tile

    def wall_copy(r, df):
        return remote(
            wall_in.at[0, planes_of(df)],
            wall_in.at[2 * r + (df != 0), planes_of(df)],
            wall_send,
            wall_recv,
            peer(-r, -df),
        )

    for r, df in around:
        wall_copy(r, df).start()
    all_walls = remote(wall_in.at[others], wall_in.at[others], wall_send, wall_recv, peer(1, 0))

    with jax.named_scope("latesweeps"):
        lax.fori_loop(EARLY_SWEEPS, SWEEPS, sweep_main, 0)

    def send_back():
        for r in range(1, num_struct):
            remote(
                main_motion.at[r, :, pl.ds(0, count_z)], back_in.at[s], back_send, back_recv, peer(r, 0)
            ).start()
        back_in[s] = main_motion[0, :, :count_z, :]

    strangers = pl.ds(0, num_struct - 1)
    all_back = remote(back_in.at[strangers], back_in.at[strangers], back_send, back_recv, peer(1, 0))
    send_back()
    wide = 2 * LANES
    lane_id = iota((LANES, wide), 0)
    group_id = iota((groups, wide), 0)

    def pair(step):
        j, k = 2 * step // count_z, 2 * step % count_z
        sums = [None] * 3
        for t in range(stencil):
            at = jnp.concatenate(
                [v_slot[t, j, pl.ds(k, 1), :], v_slot[t, j, pl.ds(k + 1, 1), :]], axis=1
            )
            by = jnp.concatenate(
                [v_weight[t, j, pl.ds(k, 1), :], v_weight[t, j, pl.ds(k + 1, 1), :]], axis=1
            )
            choose = one_hot(lane_id == at % LANES)
            values = jnp.dot(
                both[...], jnp.concatenate([choose, choose], axis=0), preferred_element_type=F32
            )
            factor = jnp.where(group_id == at // LANES, by, 0.0)
            for c in range(3):
                term = values[c * groups : (c + 1) * groups] * factor
                sums[c] = term if sums[c] is None else sums[c] + term
        for c in range(3):
            line = jnp.sum(sums[c], axis=0, keepdims=True)
            v_wall[c, pl.ds(2 * step, 1), :] = line[:, :LANES]
            v_wall[c, pl.ds(2 * step + 1, 1), :] = line[:, LANES:]

    def pairs(step, carry):
        for u in range(WALL_STEP):
            pair(step * WALL_STEP + u)
        return carry

    with jax.named_scope("wall"):
        lax.fori_loop(0, nodes // 2 // WALL_STEP, pairs, 0)

    with jax.named_scope("waitwall"):
        all_walls.wait_recv()
    with jax.named_scope("edgeinit"):
        arrived = [jnp.concatenate([wall_in[2 * r], wall_in[2 * r + 1]], axis=0) for r in range(num_struct)]
        for c in range(3):
            total = jnp.zeros((deep, LANES), F32)
            for r in range(num_struct):
                here = lane_deep // span == r
                shift = span * (r - c) - (count_z - 1)
                total = jnp.where(here & (within == 0), turn(arrived[r], shift, 1), total)
                shift = shift - count_z + far_wall
                total = jnp.where(here & (within == far_wall), turn(arrived[r], shift, 1), total)
            edge_motion[c] = total

    def sweep_edge(step, carry):
        open_forces(edge_corners(lambda c: edge_motion[c]), float_codes(edge_field[3]), work.at[0])
        fill_forces(lambda n, rows: edge_grad[n, rows], work.at[0])
        for c, value in enumerate(edge_sums()):
            edge_motion[c] = edge_motion[c] - edge_scale[c] * value
        return carry

    with jax.named_scope("sweepedge"):
        lax.fori_loop(0, SWEEPS, sweep_edge, 0)

    with jax.named_scope("waitback"):
        all_back.wait_recv()
    with jax.named_scope("outs"):
        for c in range(3):
            for j in range(count_y):
                out[c, j, :, :wall] = v_wall[c, pl.ds(j * count_z, count_z), :]
                total = None
                for q in range(num_struct):
                    moved = turn(back_in[q, c], share * q - pitch * j - SWEEPS, 1)
                    total = moved if total is None else jnp.where(lane >= share * q, moved, total)
                delta = edge_motion[c, :count_z, :]
                low = turn(delta, -1 - COLUMNS * j, 1)
                high = turn(delta, free - far_wall - COLUMNS * j, 1)
                change = jnp.where(lane < SWEEPS, low, jnp.where(lane >= free - SWEEPS, high, 0.0))
                out[c, j, :, wall:] = total + change

    with jax.named_scope("waitsend"):
        for group in (all_near, all_walls, all_back, all_packs):
            group.wait_send()


def shards(shell_motion, owner, stencil_slot, stencil_weight, prev_motion, node_offset, cell_split):
    num_struct, num_fluid = lax.axis_size("struct"), lax.axis_size("fluid")
    devices = num_struct * num_fluid
    own = shell_motion.shape[1]
    pieces = 2 * own // devices // LANES
    groups = devices * pieces
    stencil, count_y, count_z, wall = stencil_slot.shape
    total_x = prev_motion.shape[3]
    free = total_x - wall
    nodes, deep = count_y * count_z, 2 * count_z
    assert wall == free == LANES and count_z == 2 * SWEEPS == 8 and num_struct >= 2 and num_fluid >= 3
    assert num_struct * count_y * COLUMNS == LANES and 2 * stencil * nodes == LANES
    assert free // num_struct + 2 * SWEEPS <= LANES // count_y
    vmem, dma = pltpu.VMEM, pltpu.SemaphoreType.DMA
    scratch = [
        vmem((3, own), F32),
        vmem((own // LANES, LANES), jnp.int32),
        vmem((stencil, count_y, count_z, wall), jnp.int32),
        vmem((stencil, count_y, count_z, wall), F32),
        vmem((3, count_y, count_z, free), F32),
        vmem((3, count_y, count_z, total_x), F32),
        vmem((count_y, count_z, total_x), jnp.int32),
        vmem((own // LANES, LANES), jnp.int32),
        vmem((3 * groups // 2, 2 * LANES), F32),
        vmem((devices, 3 * pieces, LANES), F32),
        vmem((devices, 3 * pieces, LANES), F32),
        vmem((3 * groups, 2 * LANES), BF16),
        vmem((3, nodes, wall), F32),
        vmem((num_struct, FIELDS, count_z, LANES), F32),
        vmem((2 * num_struct, FIELDS, count_z, LANES), F32),
        vmem((2 * num_struct, count_z, LANES), F32),
        vmem((num_struct, 3, count_z, LANES), F32),
        vmem((num_struct, 4, deep, LANES), F32),
        vmem((num_struct, 3, deep, LANES), F32),
        vmem((num_struct, 54, deep, LANES), F32),
        vmem((num_struct, 3, deep, LANES), F32),
        vmem((4, deep, LANES), F32),
        vmem((3, deep, LANES), F32),
        vmem((54, deep, LANES), F32),
        vmem((3, deep, LANES), F32),
        vmem((num_struct, 2, 24, deep, LANES), F32),
        dma((7,)),
        dma,
        dma,
        dma,
        dma,
        dma,
        dma,
        dma,
        dma,
    ]
    return pl.pallas_call(
        functools.partial(window_kernel, (num_struct, num_fluid)),
        out_shape=pltpu.VMEM(prev_motion.shape, F32),
        in_specs=[pl.BlockSpec(memory_space=pltpu.HBM)] * 7,
        out_specs=pl.BlockSpec(memory_space=pltpu.VMEM),
        scratch_shapes=scratch,
        cost_estimate=pl.CostEstimate(flops=4 << 30, bytes_accessed=16 << 20, transcendentals=0),
        compiler_params=pltpu.CompilerParams(
            collective_id=0, has_side_effects=True, vmem_limit_bytes=67043328 - (1 << 17)
        ),
    )(
        shell_motion,
        owner.reshape(own // LANES, LANES),
        stencil_slot,
        stencil_weight,
        prev_motion,
        node_offset,
        cell_split,
    )


def solution(mesh):
    return jax.shard_map(
        shards,
        mesh=mesh,
        in_specs=(
            P(None, ("struct", "fluid")),
            P(("struct", "fluid"), None),
            P(None, "struct", "fluid", None),
            P(None, "struct", "fluid", None),
            P(None, "struct", "fluid", None),
            P(None, "struct", "fluid", None),
            P("struct", "fluid", None),
        ),
        out_specs=P(None, "struct", "fluid", None),
        check_vma=False,
    )
```

```python
import functools

import jax
import jax.numpy as jnp
from jax import lax
from jax.experimental import pallas as pl
from jax.experimental.pallas import tpu as pltpu
from jax.sharding import PartitionSpec as P

SWEEPS = 4
LANES = 128
LAMBDA_RATIO = 1.0
RELAX_FACTOR = 0.5
STEP_ORDERS = ((0, 1, 2), (0, 2, 1), (1, 0, 2), (1, 2, 0), (2, 0, 1), (2, 1, 0))
CORNERS = tuple((a, b, c) for a in (0, 1) for b in (0, 1) for c in (0, 1))
COLUMNS = 16
ROW_STEP = 32
WALL_STEP = 4
EARLY_PACK = 2
EARLY_SWEEPS = 2
MESH = pl.DeviceIdType.MESH
BF16 = jnp.bfloat16
F32 = jnp.float32


def split_two(values):
    high = values.astype(BF16)
    low = (values - high.astype(F32)).astype(BF16)
    return high, low


def iota(shape, dim):
    return lax.broadcasted_iota(jnp.int32, shape, dim)


def swap_corners(corners, flip_y, flip_z):
    middle = {}
    for a, b, c in CORNERS:
        middle[a, b, c] = [
            jnp.where(flip_y, q, p) for p, q in zip(corners[a, b, c], corners[a, 1 - b, c])
        ]
    return {
        (a, b, c): [jnp.where(flip_z, q, p) for p, q in zip(middle[a, b, c], middle[a, b, 1 - c])]
        for a, b, c in CORNERS
    }


def paths():
    for order in STEP_ORDERS:
        position, path = [0, 0, 0], []
        for axis_id in order:
            position[axis_id] = 1
            path.append(tuple(position))
        yield path


def cross(p, q):
    return [p[1] * q[2] - p[2] * q[1], p[2] * q[0] - p[0] * q[2], p[0] * q[1] - p[1] * q[0]]


def add_to(table, key, vector):
    table[key] = [p + q for p, q in zip(table[key], vector)] if key in table else list(vector)


RING = ((1, 0, 0), (1, 1, 0), (0, 1, 0), (0, 1, 1), (0, 0, 1), (1, 0, 1))
TOP = (1, 1, 1)


def ring_tets():
    order = [tuple(path) for path in paths()]
    for k in range(6):
        one, two = RING[k], RING[(k + 1) % 6]
        if sum(one) > sum(two):
            one, two = two, one
        yield order.index((one, two, TOP)), (one, two, TOP)


def slot_of(corner, p):
    return 3 * CORNERS.index(corner) + p


def halves(ref):
    rows = ref.shape[1]
    return [pl.ds(h, 8) for h in range(0, rows, 8)]


def finish(sums, k, give):
    done = []
    if k > 0:
        done.append(RING[k])
    if k == 5:
        done += [RING[0], TOP]
    for corner in done:
        give(corner, sums.pop(corner))


def open_gradients(offsets, flips, work):
    offsets = swap_corners(offsets, *flips)
    signs = [None] + [jnp.where(flip, -1.0, 1.0) for flip in flips]
    anchor = offsets[0, 0, 0]
    for vertex in CORNERS[1:]:
        for p in range(3):
            edge = offsets[vertex][p] - anchor[p]
            if vertex[p]:
                edge = edge + (signs[p] if p else 1.0)
            work[0, slot_of(vertex, p)] = edge


def fill_gradients(work, put):
    for rows in halves(work.at[0]):
        sums = {}
        for k, (tet, path) in enumerate(ring_tets()):
            one, two, three = [[work[0, slot_of(v, p), rows] for p in range(3)] for v in path]
            across = [cross(two, three), cross(three, one), cross(one, two)]
            inverse = 1.0 / (one[0] * across[0][0] + one[1] * across[0][1] + one[2] * across[0][2])
            grads = [[p * inverse for p in vector] for vector in across]
            for v in range(3):
                for p in range(3):
                    put(9 * tet + 3 * v + p, rows, grads[v][p])
            first = [grads[0][p] + grads[1][p] + grads[2][p] for p in range(3)]
            for vertex, grad in zip(((0, 0, 0),) + path, [first] + grads):
                square = [p * p for p in grad]
                norm = square[0] + square[1] + square[2]
                add_to(sums, vertex, [(LAMBDA_RATIO + 1.0) * p + norm for p in square])

            def give(corner, vector):
                for p in range(3):
                    work[1, slot_of(corner, p), rows] = vector[p]

            finish(sums, k, give)
        give((0, 0, 0), sums[0, 0, 0])


def close_cells(work, flips):
    parts = swap_corners({v: [work[1, slot_of(v, p)] for p in range(3)] for v in CORNERS}, *flips)
    return {
        (a, b): [p + turn(q, 1, 0) for p, q in zip(parts[a, b, 0], parts[a, b, 1])]
        for a in (0, 1)
        for b in (0, 1)
    }


def open_forces(motion, flips, work):
    motion = swap_corners(motion, *flips)
    anchor = motion[0, 0, 0]
    for vertex in CORNERS[1:]:
        for p in range(3):
            work[0, slot_of(vertex, p)] = motion[vertex][p] - anchor[p]


def fill_forces(get, work):
    for rows in halves(work.at[0]):
        sums, total = {}, [None]
        top = [work[0, slot_of(TOP, p), rows] for p in range(3)]
        for k, (tet, path) in enumerate(ring_tets()):
            grads = [[get(9 * tet + 3 * v + p, rows) for p in range(3)] for v in range(3)]
            moves = [[work[0, slot_of(v, p), rows] for p in range(3)] for v in path[:2]] + [top]
            tensor = [
                [
                    moves[0][p] * grads[0][q] + moves[1][p] * grads[1][q] + moves[2][p] * grads[2][q]
                    for q in range(3)
                ]
                for p in range(3)
            ]
            trace = LAMBDA_RATIO * (tensor[0][0] + tensor[1][1] + tensor[2][2])
            stress = [[None] * 3 for _ in range(3)]
            for p in range(3):
                stress[p][p] = tensor[p][p] + tensor[p][p] + trace
                for q in range(p):
                    stress[p][q] = stress[q][p] = tensor[p][q] + tensor[q][p]
            for v in range(3):
                add_to(
                    sums,
                    path[v],
                    [
                        stress[p][0] * grads[v][0] + stress[p][1] * grads[v][1] + stress[p][2] * grads[v][2]
                        for p in range(3)
                    ],
                )

            def give(corner, vector):
                for p in range(3):
                    work[1, slot_of(corner, p), rows] = vector[p]
                total[0] = vector if total[0] is None else [p + q for p, q in zip(total[0], vector)]

            finish(sums, k, give)
        for p in range(3):
            work[1, p, rows] = -total[0][p]


def turn(x, shift, axis):
    shift %= x.shape[axis]
    return pltpu.roll(x, shift, axis) if shift else x


def float_codes(value):
    return value >= 1.5, (value == 1.0) | (value == 3.0)


def with_planes(edges):
    corners = {}
    for (a, b), values in edges.items():
        corners[a, b, 0] = values
        corners[a, b, 1] = [turn(p, -1, 0) for p in values]
    return corners


def one_hot(mask):
    return mask.astype(F32).astype(BF16)


def exact_ids(count, width):
    return iota((count, width), 0).astype(F32).astype(BF16)


def equal_hot(ids, row):
    row = jnp.broadcast_to(row.astype(F32), (16, row.shape[1])).astype(BF16)
    row = jnp.concatenate([row] * (ids.shape[0] // 16), axis=0)
    return jnp.where(ids == row, jnp.ones_like(ids), jnp.zeros_like(ids))


def place_nodes(devices, capacity, own_ref, place_ref):
    rows = own_ref.shape[0]
    own = own_ref[...]
    upper = iota((LANES, LANES), 0) < iota((LANES, LANES), 1)
    prefix = jnp.concatenate([one_hot(upper), jnp.ones((LANES, LANES), BF16)], axis=0)
    lower = one_hot(iota((rows, rows), 1) < iota((rows, rows), 0))
    chunk = min(devices, 8)

    def ranks(step, place):
        masks = [own == step * chunk + o for o in range(chunk)]
        named = [one_hot(mask) for mask in masks]
        above = jnp.dot(lower, jnp.concatenate(named, axis=1), preferred_element_type=F32).astype(BF16)
        left = [
            jnp.concatenate([named[o], above[:, o * LANES : (o + 1) * LANES]], axis=1) for o in range(chunk)
        ]
        rank = jnp.dot(jnp.concatenate(left, axis=0), prefix, preferred_element_type=F32)
        for o in range(chunk):
            base = ((step * chunk + o) * capacity) * 1.0
            place = jnp.where(masks[o], rank[o * rows : (o + 1) * rows] + base, place)
        return place

    place = jnp.zeros((rows, LANES), F32)
    if devices <= 4 * chunk:
        for step in range(devices // chunk):
            place = ranks(step, place)
    else:
        place = lax.fori_loop(0, devices // chunk, ranks, place)
    place_ref[...] = place.astype(jnp.int32)


def pack_nodes(first, last, place_ref, val_ref, acc_ref):
    wide = 2 * LANES
    groups = acc_ref.shape[0] // 3
    pair = 16
    group_id = exact_ids(groups, LANES)
    lane_id = exact_ids(wide, LANES)

    def spread(step, carry):
        columns, parts = [], [[] for _ in range(6)]
        for u in range(ROW_STEP):
            row = step * ROW_STEP + u
            at = place_ref[pl.ds(row, 1), :]
            hit = equal_hot(group_id, at // wide)
            columns.append(equal_hot(lane_id, at % wide))
            for c in range(3):
                value = val_ref[pl.ds(c, 1), pl.ds(pl.multiple_of(row * LANES, LANES), LANES)]
                value = jnp.broadcast_to(value, (pair, LANES))
                high = value.astype(BF16)
                low = (value - high.astype(F32)).astype(BF16)
                for n, part in ((c, high), (3 + c, low)):
                    parts[n].append(hit * jnp.concatenate([part] * (groups // pair), axis=0))
        left = jnp.concatenate([jnp.concatenate(part, axis=1) for part in parts], axis=0)
        right = jnp.concatenate(columns, axis=1)
        product = lax.dot_general(left, right, (((1,), (1,)), ((), ())), preferred_element_type=F32)
        acc_ref[...] += product[: 3 * groups] + product[3 * groups :]
        return carry

    lax.fori_loop(first, last, spread, 0)


def strips(num_struct, count_y, free):
    strip = free // num_struct + 2 * SWEEPS
    per_tile = LANES // strip
    return strip, per_tile, -(-num_struct * count_y // per_tile), -(-7 * count_y // per_tile)


def window_kernel(
    counts,
    shell,
    owner,
    slot,
    weight,
    prev,
    offset,
    split,
    out,
    v_shell,
    v_owner,
    v_slot,
    v_weight,
    v_prev,
    v_offset,
    v_split,
    place,
    acc,
    packed,
    received,
    both,
    v_wall,
    tiles,
    near_in,
    edge_in,
    wall_in,
    back_out,
    back_in,
    main_field,
    main_motion,
    main_grad,
    main_scale,
    edge_field,
    edge_motion,
    edge_grad,
    edge_scale,
    work,
    local_sem,
    near_send,
    near_recv,
    edge_send,
    edge_recv,
    pack_send,
    pack_recv,
    wall_send,
    wall_recv,
    back_send,
    back_recv,
):
    num_struct, num_fluid = counts
    devices = num_struct * num_fluid
    s, f = lax.axis_index("struct"), lax.axis_index("fluid")
    me = s * num_fluid + f
    stencil, count_y, count_z, wall = slot.shape
    free = prev.shape[3] - wall
    nodes = count_y * count_z
    deep = 2 * count_z
    span = count_y * COLUMNS
    share = free // num_struct
    rows_all = num_struct * count_y
    strip, per_tile, main_tiles, near_tiles = strips(num_struct, count_y, free)
    rows_own = v_owner.shape[0]
    capacity = 2 * rows_own * LANES // devices
    pieces = capacity // LANES
    groups = devices * pieces
    far_wall = 2 * SWEEPS + SWEEPS + 1

    def peer(ds, df):
        return ((s + ds + num_struct) % num_struct, (f + df + num_fluid) % num_fluid)

    def remote(src, dst, send, recv, where):
        return pltpu.make_async_remote_copy(
            src_ref=src, dst_ref=dst, send_sem=send, recv_sem=recv, device_id=where, device_id_type=MESH
        )

    loads = [
        (owner, v_owner),
        (offset, v_offset),
        (split, v_split),
        (prev.at[:, :, :, pl.ds(wall, free)], v_prev),
        (shell, v_shell),
        (slot, v_slot),
        (weight, v_weight),
    ]
    loads = [pltpu.make_async_copy(a, b, local_sem.at[n]) for n, (a, b) in enumerate(loads)]
    for load in loads:
        load.start()

    barrier = pltpu.get_barrier_semaphore()

    shifts = sorted(range(num_fluid), key=lambda d: -min(d, num_fluid - d))
    everyone = [peer(ds, df) for ds in range(num_struct) for df in shifts if (ds, df) != (0, 0)]
    for to in everyone:
        pl.semaphore_signal(barrier, inc=1, device_id=to, device_id_type=MESH)

    with jax.named_scope("place"):
        loads[0].wait()
        place_nodes(devices, capacity, v_owner, place)

    lane = iota((count_z, LANES), 1)
    with jax.named_scope("tiles"):
        for load in loads[1:4]:
            load.wait()
        slab = jnp.zeros((count_z, LANES), F32)
        joined = [[None] * near_tiles for _ in range(num_struct)]
        for n in range(7):
            for j in range(count_y):
                if n < 3:
                    near, far = v_offset[n, j, :, :wall], v_offset[n, j, :, wall:]
                elif n == 3:
                    near, far = v_split[j, :, :wall].astype(F32), v_split[j, :, wall:].astype(F32)
                else:
                    near, far = jnp.zeros((count_z, LANES), F32), v_prev[n - 4, j]
                for q in range(num_struct):
                    begin = share * q - SWEEPS
                    line = far
                    if begin < 0:
                        line = jnp.where(lane >= LANES + begin, near, far)
                    if begin + strip > LANES:
                        line = jnp.where(lane < begin + strip - LANES, near, far)
                    t, m = divmod(n * count_y + j, per_tile)
                    line = turn(line, strip * m - begin, 1)
                    joined[q][t] = jnp.where(lane >= strip * m, line, joined[q][t]) if m else line
                if n < 4:
                    base = span * n + COLUMNS * j
                    low = turn(jnp.where(lane == LANES - 1, near, far), base + 1, 1)
                    high = turn(jnp.where(lane == 0, near, far), base + far_wall, 1)
                    slab = jnp.where((lane >= base) & (lane < base + 2 * SWEEPS), low, slab)
                    slab = jnp.where(
                        (lane >= base + 2 * SWEEPS) & (lane < base + COLUMNS), high, slab
                    )
        for q in range(num_struct):
            for t in range(near_tiles):
                tiles[q, t] = joined[q][t]
        edge_in[0] = slab

    steps = rows_own // ROW_STEP
    with jax.named_scope("packfirst"):
        acc[...] = jnp.zeros_like(acc)
        loads[4].wait()
        pack_nodes(0, EARLY_PACK, place, v_shell, acc)
    with jax.named_scope("barrier"):
        pl.semaphore_wait(barrier, devices - 1)

    around = [(r, df) for r in range(num_struct) for df in (0, -1, 1) if (r, df) != (0, 0)]

    def planes_of(df):
        return pl.ds(0, count_z) if df == 0 else pl.ds(0 if df > 0 else SWEEPS, SWEEPS)

    def near_copy(r, df):
        to = peer(-r, -df)
        return remote(
            tiles.at[to[0], :, planes_of(df)],
            near_in.at[2 * r + (df != 0), :, planes_of(df)],
            near_send,
            near_recv,
            to,
        )

    others = pl.ds(1, 2 * num_struct - 1)
    def spread_copy(buffer, send, recv, r, df):
        return remote(
            buffer.at[0, planes_of(df)],
            buffer.at[2 * r + (df != 0), planes_of(df)],
            send,
            recv,
            peer(-r, -df),
        )

    def send_around(buffer, send, recv):
        for r, df in around:
            spread_copy(buffer, send, recv, r, df).start()
        return remote(buffer.at[others], buffer.at[others], send, recv, peer(1, 0))

    all_edges = send_around(edge_in, edge_send, edge_recv)
    for r, df in around:
        near_copy(r, df).start()
    all_near = remote(near_in.at[others], near_in.at[others], near_send, near_recv, peer(1, 0))
    near_in[0] = tiles[s]


    with jax.named_scope("pack"):
        pack_nodes(EARLY_PACK, steps, place, v_shell, acc)
    with jax.named_scope("relay"):
        pack_groups = groups // 2
        for o in range(devices):
            for c in range(3):
                for b in range(pieces):
                    m = o * pieces + b
                    packed[o, pl.ds(c * pieces + b, 1), :] = acc[
                        pl.ds(c * pack_groups + m // 2, 1), pl.ds((m % 2) * LANES, LANES)
                    ]

    with jax.named_scope("sendpack"):

        for to in everyone:
            remote(packed.at[to[0] * num_fluid + to[1]], received.at[me], pack_send, pack_recv, to).start()
        received[me] = packed[me]
    all_packs = remote(
        packed.at[pl.ds(0, devices - 1)],
        received.at[pl.ds(0, devices - 1)],
        pack_send,
        pack_recv,
        peer(1, 0),
    )

    lane_deep = iota((deep, LANES), 1)
    column = lane_deep % strip + share * s
    within = lane_deep % COLUMNS
    inner = ((within >= 1) & (within <= SWEEPS)) | ((within > 2 * SWEEPS) & (within < far_wall))
    free_node = (column >= SWEEPS) & (column < free + SWEEPS) & (lane_deep < strip * per_tile)

    tail = [strip * (min(per_tile, rows_all - per_tile * t) - 1) for t in range(main_tiles)]

    def main_corners(read):
        values = [[read(t, c) for c in range(3)] for t in range(main_tiles)]
        for t, here in enumerate(values):
            following = values[(t + 1) % main_tiles]
            high = [
                [
                    jnp.where(lane_deep < tail[t], turn(p, -strip - a, 1), turn(q, tail[t] - a, 1))
                    for p, q in zip(here, following)
                ]
                for a in (0, 1)
            ]
            near = [turn(p, -1, 1) for p in here]
            yield t, with_planes({(0, 0): here, (1, 0): near, (0, 1): high[0], (1, 1): high[1]})

    def main_sums():
        lows, insides, outsides = [], [], []
        for t in range(main_tiles):
            ends = close_cells(work.at[t], float_codes(main_field[t, 3]))
            lows.append([p + turn(q, 1, 1) for p, q in zip(ends[0, 0], ends[1, 0])])
            upper = list(zip(ends[0, 1], ends[1, 1]))
            insides.append([turn(p, strip, 1) + turn(q, strip + 1, 1) for p, q in upper])
            outsides.append([turn(p, -tail[t], 1) + turn(q, 1 - tail[t], 1) for p, q in upper])
        for t in range(main_tiles):
            yield t, [
                p + jnp.where(lane_deep < strip, before, now)
                for p, before, now in zip(lows[t], outsides[t - 1], insides[t])
            ]

    def prepare_main():
        source = [
            [jnp.concatenate([near_in[2 * r, t], near_in[2 * r + 1, t]], axis=0) for t in range(near_tiles)]
            for r in range(num_struct)
        ]
        for n in range(7):
            for t in range(main_tiles):
                total = None
                for m in range(min(per_tile, rows_all - per_tile * t)):
                    r, j = divmod(per_tile * t + m, count_y)
                    k, at = divmod(n * count_y + j, per_tile)
                    moved = turn(source[r][k], strip * (m - at), 1)
                    total = jnp.where(lane_deep >= strip * m, moved, total) if m else moved
                if n < 4:
                    main_field[t, n] = total
                else:
                    main_motion[t, n - 4] = total
        for r, corners in main_corners(lambda at, c: main_field[at, c]):
            open_gradients(corners, float_codes(main_field[r, 3]), work.at[r])

        def row(r, carry):
            def put(n, rows, value):
                main_grad[r, n, rows] = value

            fill_gradients(work.at[r], put)
            return carry

        lax.fori_loop(0, main_tiles, row, 0)
        for r, values in main_sums():
            for c in range(3):
                main_scale[r, c] = jnp.where(free_node, RELAX_FACTOR / values[c], 0.0)

    def sweep_main(sweep, carry):
        for r, corners in main_corners(lambda at, c: main_motion[at, c]):
            open_forces(corners, float_codes(main_field[r, 3]), work.at[r])

        for r in range(main_tiles):
            fill_forces(lambda n, rows: main_grad[r, n, rows], work.at[r])
        for r, values in main_sums():
            for c in range(3):
                main_motion[r, c] = main_motion[r, c] - main_scale[r, c] * values[c]
        return carry

    def edge_corners(read):
        values = [read(c) for c in range(3)]
        return with_planes(
            {(a, b): [turn(p, -a - COLUMNS * b, 1) for p in values] for a in (0, 1) for b in (0, 1)}
        )

    def edge_sums():
        ends = close_cells(work.at[0], float_codes(edge_field[3]))
        moved = [[turn(p, a + COLUMNS * b, 1) for p in ends[a, b]] for a in (0, 1) for b in (0, 1)]
        return [(p + q) + (u + v) for p, q, u, v in zip(*moved)]

    def prepare_edge():
        for r in range(num_struct):
            whole = jnp.concatenate([edge_in[2 * r], edge_in[2 * r + 1]], axis=0)
            for n in range(4):
                moved = turn(whole, span * (r - n), 1)
                if r > 0:
                    moved = jnp.where(lane_deep >= span * r, moved, edge_field[n])
                edge_field[n] = moved
        open_gradients(edge_corners(lambda c: edge_field[c]), float_codes(edge_field[3]), work.at[0])

        def put(n, rows, value):
            edge_grad[n, rows] = value

        fill_gradients(work.at[0], put)
        for c, value in enumerate(edge_sums()):
            edge_scale[c] = jnp.where(inner, RELAX_FACTOR / value, 0.0)

    def plane_points(ref, zero):
        row, at = iota((nodes, LANES), 0), iota((nodes, LANES), 1)
        within = row // count_z * (2 * count_z) + count_z - 1 - row % count_z
        total = None
        for t in range(stencil):
            whole = jnp.concatenate([ref[t, j] for j in range(count_y)], axis=0)
            for side in (0, 1):
                edge = wall - 1 if side == 0 else 0
                spread = jnp.broadcast_to(whole[:, edge : edge + 1], (nodes, LANES))
                part = jnp.where(at == 2 * nodes * t + count_z * side + within, spread, zero)
                total = part if total is None else total + part
        return jnp.sum(total, axis=0, keepdims=True)

    with jax.named_scope("prepedge"):
        all_edges.wait_recv()
        prepare_edge()
    with jax.named_scope("points"):
        loads[5].wait()
        loads[6].wait()
        plane_slot, plane_weight = plane_points(v_slot, 0), plane_points(v_weight, 0.0)

    with jax.named_scope("waitnear"):
        all_near.wait_recv()
    with jax.named_scope("prepmain"):
        prepare_main()
    with jax.named_scope("sweeps"):
        lax.fori_loop(0, EARLY_SWEEPS, sweep_main, 0)
    with jax.named_scope("waitpack"):
        all_packs.wait_recv()

    with jax.named_scope("table"):
        for c in range(3):
            whole = jnp.concatenate(
                [received[o, pl.ds(c * pieces, pieces), :] for o in range(devices)], axis=0
            )
            high, low = split_two(whole)
            both[pl.ds(c * groups, groups), :LANES] = high
            both[pl.ds(c * groups, groups), LANES:] = low

    with jax.named_scope("planes"):
        pick = one_hot(iota((LANES, LANES), 0) == plane_slot % LANES)
        found = jnp.dot(both[...], jnp.concatenate([pick, pick], axis=0), preferred_element_type=F32)
        scaled = jnp.where(iota((groups, LANES), 0) == plane_slot // LANES, plane_weight, 0.0)
        tile = jnp.zeros((count_z, LANES), F32)
        for c in range(3):
            line = jnp.sum(found[c * groups : (c + 1) * groups] * scaled, axis=0, keepdims=True)
            period = LANES // 2
            while period >= 2 * nodes:
                line = line + turn(line, period, 1)
                period //= 2
            spread = pltpu.roll(jnp.broadcast_to(line, (count_z, LANES)), 0, 1, stride=1, stride_axis=0)
            tile = jnp.where((lane >= span * c) & (lane < span * (c + 1)), spread, tile)
        wall_in[0] = tile

    all_walls = send_around(wall_in, wall_send, wall_recv)

    with jax.named_scope("latesweeps"):
        lax.fori_loop(EARLY_SWEEPS, SWEEPS, sweep_main, 0)

    def send_back():
        for r in range(num_struct):
            for c in range(3):
                total = None
                for j in range(count_y):
                    t, m = divmod(r * count_y + j, per_tile)
                    moved = turn(main_motion[t, c, :count_z, :], strip * (j - m), 1)
                    total = jnp.where(lane >= strip * j, moved, total) if j else moved
                back_out[r, c] = total
        for r in range(1, num_struct):
            remote(back_out.at[r], back_in.at[s], back_send, back_recv, peer(r, 0)).start()
        back_in[s] = back_out[0]

    strangers = pl.ds(0, num_struct - 1)
    all_back = remote(back_in.at[strangers], back_in.at[strangers], back_send, back_recv, peer(1, 0))
    send_back()
    wide = 2 * LANES
    lane_id = exact_ids(LANES, wide)
    group_id = iota((groups, wide), 0)

    def pair(step):
        j, k = 2 * step // count_z, 2 * step % count_z
        sums = [None] * 3
        for t in range(stencil):
            at = jnp.concatenate(
                [v_slot[t, j, pl.ds(k, 1), :], v_slot[t, j, pl.ds(k + 1, 1), :]], axis=1
            )
            by = jnp.concatenate(
                [v_weight[t, j, pl.ds(k, 1), :], v_weight[t, j, pl.ds(k + 1, 1), :]], axis=1
            )
            choose = equal_hot(lane_id, at % LANES)
            values = jnp.dot(
                both[...], jnp.concatenate([choose, choose], axis=0), preferred_element_type=F32
            )
            factor = jnp.where(group_id == at // LANES, by, 0.0)
            for c in range(3):
                term = values[c * groups : (c + 1) * groups] * factor
                sums[c] = term if sums[c] is None else sums[c] + term
        for c in range(3):
            line = jnp.sum(sums[c], axis=0, keepdims=True)
            v_wall[c, pl.ds(2 * step, 1), :] = line[:, :LANES]
            v_wall[c, pl.ds(2 * step + 1, 1), :] = line[:, LANES:]

    def pairs(step, carry):
        for u in range(WALL_STEP):
            pair(step * WALL_STEP + u)
        return carry

    with jax.named_scope("wall"):
        lax.fori_loop(0, nodes // 2 // WALL_STEP, pairs, 0)

    with jax.named_scope("waitwall"):
        all_walls.wait_recv()
    with jax.named_scope("edgeinit"):
        arrived = [jnp.concatenate([wall_in[2 * r], wall_in[2 * r + 1]], axis=0) for r in range(num_struct)]
        for c in range(3):
            total = jnp.zeros((deep, LANES), F32)
            for r in range(num_struct):
                here = lane_deep // span == r
                shift = span * (r - c) - (count_z - 1)
                total = jnp.where(here & (within == 0), turn(arrived[r], shift, 1), total)
                shift = shift - count_z + far_wall
                total = jnp.where(here & (within == far_wall), turn(arrived[r], shift, 1), total)
            edge_motion[c] = total

    def sweep_edge(step, carry):
        open_forces(edge_corners(lambda c: edge_motion[c]), float_codes(edge_field[3]), work.at[0])
        fill_forces(lambda n, rows: edge_grad[n, rows], work.at[0])
        for c, value in enumerate(edge_sums()):
            edge_motion[c] = edge_motion[c] - edge_scale[c] * value
        return carry

    with jax.named_scope("sweepedge"):
        lax.fori_loop(0, SWEEPS, sweep_edge, 0)

    with jax.named_scope("waitback"):
        all_back.wait_recv()
    with jax.named_scope("outs"):
        for c in range(3):
            for j in range(count_y):
                out[c, j, :, :wall] = v_wall[c, pl.ds(j * count_z, count_z), :]
                total = None
                for q in range(num_struct):
                    moved = turn(back_in[q, c], share * q - strip * j - SWEEPS, 1)
                    total = moved if total is None else jnp.where(lane >= share * q, moved, total)
                delta = edge_motion[c, :count_z, :]
                low = turn(delta, -1 - COLUMNS * j, 1)
                high = turn(delta, free - far_wall - COLUMNS * j, 1)
                change = jnp.where(lane < SWEEPS, low, jnp.where(lane >= free - SWEEPS, high, 0.0))
                out[c, j, :, wall:] = total + change

    with jax.named_scope("waitsend"):
        for group in (all_near, all_edges, all_walls, all_back, all_packs):
            group.wait_send()


def shards(shell_motion, owner, stencil_slot, stencil_weight, prev_motion, node_offset, cell_split):
    num_struct, num_fluid = lax.axis_size("struct"), lax.axis_size("fluid")
    devices = num_struct * num_fluid
    own = shell_motion.shape[1]
    pieces = 2 * own // devices // LANES
    groups = devices * pieces
    stencil, count_y, count_z, wall = stencil_slot.shape
    total_x = prev_motion.shape[3]
    free = total_x - wall
    nodes, deep = count_y * count_z, 2 * count_z
    assert wall == free == LANES and count_z == 2 * SWEEPS == 8 and num_struct >= 2 and num_fluid >= 3
    assert num_struct * count_y * COLUMNS == LANES and 2 * stencil * nodes == LANES
    strip, per_tile, main_tiles, near_tiles = strips(num_struct, count_y, free)
    assert count_y <= per_tile and num_struct * count_y > per_tile
    vmem, dma = pltpu.VMEM, pltpu.SemaphoreType.DMA
    scratch = [
        vmem((3, own), F32),
        vmem((own // LANES, LANES), jnp.int32),
        vmem((stencil, count_y, count_z, wall), jnp.int32),
        vmem((stencil, count_y, count_z, wall), F32),
        vmem((3, count_y, count_z, free), F32),
        vmem((3, count_y, count_z, total_x), F32),
        vmem((count_y, count_z, total_x), jnp.int32),
        vmem((own // LANES, LANES), jnp.int32),
        vmem((3 * groups // 2, 2 * LANES), F32),
        vmem((devices, 3 * pieces, LANES), F32),
        vmem((devices, 3 * pieces, LANES), F32),
        vmem((3 * groups, 2 * LANES), BF16),
        vmem((3, nodes, wall), F32),
        vmem((num_struct, near_tiles, count_z, LANES), F32),
        vmem((2 * num_struct, near_tiles, count_z, LANES), F32),
        vmem((2 * num_struct, count_z, LANES), F32),
        vmem((2 * num_struct, count_z, LANES), F32),
        vmem((num_struct, 3, count_z, LANES), F32),
        vmem((num_struct, 3, count_z, LANES), F32),
        vmem((main_tiles, 4, deep, LANES), F32),
        vmem((main_tiles, 3, deep, LANES), F32),
        vmem((main_tiles, 54, deep, LANES), F32),
        vmem((main_tiles, 3, deep, LANES), F32),
        vmem((4, deep, LANES), F32),
        vmem((3, deep, LANES), F32),
        vmem((54, deep, LANES), F32),
        vmem((3, deep, LANES), F32),
        vmem((main_tiles, 2, 24, deep, LANES), F32),
        dma((7,)),
        dma,
        dma,
        dma,
        dma,
        dma,
        dma,
        dma,
        dma,
        dma,
        dma,
    ]
    return pl.pallas_call(
        functools.partial(window_kernel, (num_struct, num_fluid)),
        out_shape=pltpu.VMEM(prev_motion.shape, F32),
        in_specs=[pl.BlockSpec(memory_space=pltpu.HBM)] * 7,
        out_specs=pl.BlockSpec(memory_space=pltpu.VMEM),
        scratch_shapes=scratch,
        cost_estimate=pl.CostEstimate(flops=4 << 30, bytes_accessed=16 << 20, transcendentals=0),
        compiler_params=pltpu.CompilerParams(
            collective_id=0, has_side_effects=True, vmem_limit_bytes=67043328 - (1 << 17)
        ),
    )(
        shell_motion,
        owner.reshape(own // LANES, LANES),
        stencil_slot,
        stencil_weight,
        prev_motion,
        node_offset,
        cell_split,
    )


def solution(mesh):
    return jax.shard_map(
        shards,
        mesh=mesh,
        in_specs=(
            P(None, ("struct", "fluid")),
            P(("struct", "fluid"), None),
            P(None, "struct", "fluid", None),
            P(None, "struct", "fluid", None),
            P(None, "struct", "fluid", None),
            P(None, "struct", "fluid", None),
            P("struct", "fluid", None),
        ),
        out_specs=P(None, "struct", "fluid", None),
        check_vma=False,
    )
```

```python
import functools

import jax
import jax.numpy as jnp
from jax import lax
from jax.experimental import pallas as pl
from jax.experimental.pallas import tpu as pltpu
from jax.sharding import PartitionSpec as P

SWEEPS = 4
LANES = 128
LAMBDA_RATIO = 1.0
RELAX_FACTOR = 0.5
STEP_ORDERS = ((0, 1, 2), (0, 2, 1), (1, 0, 2), (1, 2, 0), (2, 0, 1), (2, 1, 0))
CORNERS = tuple((a, b, c) for a in (0, 1) for b in (0, 1) for c in (0, 1))
COLUMNS = 16
ROW_STEP = 32
WALL_STEP = 8
EARLY_SWEEPS = 2
MESH = pl.DeviceIdType.MESH
BF16 = jnp.bfloat16
F32 = jnp.float32


def split_two(values):
    high = values.astype(BF16)
    low = (values - high.astype(F32)).astype(BF16)
    return high, low


def iota(shape, dim):
    return lax.broadcasted_iota(jnp.int32, shape, dim)


def swap_corners(corners, flip_y, flip_z):
    middle = {}
    for a, b, c in CORNERS:
        middle[a, b, c] = [
            jnp.where(flip_y, q, p) for p, q in zip(corners[a, b, c], corners[a, 1 - b, c])
        ]
    return {
        (a, b, c): [jnp.where(flip_z, q, p) for p, q in zip(middle[a, b, c], middle[a, b, 1 - c])]
        for a, b, c in CORNERS
    }


def paths():
    for order in STEP_ORDERS:
        position, path = [0, 0, 0], []
        for axis_id in order:
            position[axis_id] = 1
            path.append(tuple(position))
        yield path


def cross(p, q):
    return [p[1] * q[2] - p[2] * q[1], p[2] * q[0] - p[0] * q[2], p[0] * q[1] - p[1] * q[0]]


def add_to(table, key, vector):
    table[key] = [p + q for p, q in zip(table[key], vector)] if key in table else list(vector)


RING = ((1, 0, 0), (1, 1, 0), (0, 1, 0), (0, 1, 1), (0, 0, 1), (1, 0, 1))
TOP = (1, 1, 1)


def ring_tets():
    order = [tuple(path) for path in paths()]
    for k in range(6):
        one, two = RING[k], RING[(k + 1) % 6]
        if sum(one) > sum(two):
            one, two = two, one
        yield order.index((one, two, TOP)), (one, two, TOP)


def slot_of(corner, p):
    return 3 * CORNERS.index(corner) + p


def halves(ref):
    rows = ref.shape[1]
    return [pl.ds(h, 8) for h in range(0, rows, 8)]


def finish(sums, k, give):
    done = []
    if k > 0:
        done.append(RING[k])
    if k == 5:
        done += [RING[0], TOP]
    for corner in done:
        give(corner, sums.pop(corner))


def open_gradients(offsets, flips, work):
    offsets = swap_corners(offsets, *flips)
    signs = [None] + [jnp.where(flip, -1.0, 1.0) for flip in flips]
    anchor = offsets[0, 0, 0]
    for vertex in CORNERS[1:]:
        for p in range(3):
            edge = offsets[vertex][p] - anchor[p]
            if vertex[p]:
                edge = edge + (signs[p] if p else 1.0)
            work[0, slot_of(vertex, p)] = edge


def fill_gradients(work, put):
    for rows in halves(work.at[0]):
        sums = {}
        for k, (tet, path) in enumerate(ring_tets()):
            one, two, three = [[work[0, slot_of(v, p), rows] for p in range(3)] for v in path]
            across = [cross(two, three), cross(three, one), cross(one, two)]
            inverse = 1.0 / (one[0] * across[0][0] + one[1] * across[0][1] + one[2] * across[0][2])
            grads = [[p * inverse for p in vector] for vector in across]
            for v in range(3):
                for p in range(3):
                    put(9 * tet + 3 * v + p, rows, grads[v][p])
            first = [grads[0][p] + grads[1][p] + grads[2][p] for p in range(3)]
            for vertex, grad in zip(((0, 0, 0),) + path, [first] + grads):
                square = [p * p for p in grad]
                norm = square[0] + square[1] + square[2]
                add_to(sums, vertex, [(LAMBDA_RATIO + 1.0) * p + norm for p in square])

            def give(corner, vector):
                for p in range(3):
                    work[1, slot_of(corner, p), rows] = vector[p]

            finish(sums, k, give)
        give((0, 0, 0), sums[0, 0, 0])


def close_cells(work, flips):
    parts = swap_corners({v: [work[1, slot_of(v, p)] for p in range(3)] for v in CORNERS}, *flips)
    return {
        (a, b): [p + turn(q, 1, 0) for p, q in zip(parts[a, b, 0], parts[a, b, 1])]
        for a in (0, 1)
        for b in (0, 1)
    }


def open_forces(motion, flips, work):
    motion = swap_corners(motion, *flips)
    anchor = motion[0, 0, 0]
    for vertex in CORNERS[1:]:
        for p in range(3):
            work[0, slot_of(vertex, p)] = motion[vertex][p] - anchor[p]


def fill_forces(get, work):
    for rows in halves(work.at[0]):
        sums, total = {}, [None]
        top = [work[0, slot_of(TOP, p), rows] for p in range(3)]
        for k, (tet, path) in enumerate(ring_tets()):
            grads = [[get(9 * tet + 3 * v + p, rows) for p in range(3)] for v in range(3)]
            moves = [[work[0, slot_of(v, p), rows] for p in range(3)] for v in path[:2]] + [top]
            tensor = [
                [
                    moves[0][p] * grads[0][q] + moves[1][p] * grads[1][q] + moves[2][p] * grads[2][q]
                    for q in range(3)
                ]
                for p in range(3)
            ]
            trace = LAMBDA_RATIO * (tensor[0][0] + tensor[1][1] + tensor[2][2])
            stress = [[None] * 3 for _ in range(3)]
            for p in range(3):
                stress[p][p] = tensor[p][p] + tensor[p][p] + trace
                for q in range(p):
                    stress[p][q] = stress[q][p] = tensor[p][q] + tensor[q][p]
            for v in range(3):
                add_to(
                    sums,
                    path[v],
                    [
                        stress[p][0] * grads[v][0] + stress[p][1] * grads[v][1] + stress[p][2] * grads[v][2]
                        for p in range(3)
                    ],
                )

            def give(corner, vector):
                for p in range(3):
                    work[1, slot_of(corner, p), rows] = vector[p]
                total[0] = vector if total[0] is None else [p + q for p, q in zip(total[0], vector)]

            finish(sums, k, give)
        for p in range(3):
            work[1, p, rows] = -total[0][p]


def turn(x, shift, axis):
    shift %= x.shape[axis]
    return pltpu.roll(x, shift, axis) if shift else x


def float_codes(value):
    return value >= 1.5, (value == 1.0) | (value == 3.0)


def with_planes(edges):
    corners = {}
    for (a, b), values in edges.items():
        corners[a, b, 0] = values
        corners[a, b, 1] = [turn(p, -1, 0) for p in values]
    return corners


def one_hot(mask):
    return mask.astype(F32).astype(BF16)


def exact_ids(count, width):
    return iota((count, width), 0).astype(F32).astype(BF16)


def equal_hot(ids, row):
    row = jnp.broadcast_to(row.astype(F32), (16, row.shape[1])).astype(BF16)
    row = jnp.concatenate([row] * (ids.shape[0] // 16), axis=0)
    return jnp.where(ids == row, jnp.ones_like(ids), jnp.zeros_like(ids))


def place_nodes(devices, capacity, own_ref, place_ref):
    rows = own_ref.shape[0]
    own = own_ref[...]
    ids = own.astype(F32).astype(BF16)
    upper = iota((LANES, LANES), 0) < iota((LANES, LANES), 1)
    prefix = jnp.concatenate([one_hot(upper), jnp.ones((LANES, LANES), BF16)], axis=0)
    lower = one_hot(iota((rows, rows), 1) < iota((rows, rows), 0))
    chunk = min(devices, 8)

    def ranks(step, place):
        masks = [own == step * chunk + o for o in range(chunk)]
        named = [
            jnp.where(ids == (step * chunk + o) * 1.0, jnp.ones_like(ids), jnp.zeros_like(ids))
            for o in range(chunk)
        ]
        above = jnp.dot(lower, jnp.concatenate(named, axis=1), preferred_element_type=F32).astype(BF16)
        left = [
            jnp.concatenate([named[o], above[:, o * LANES : (o + 1) * LANES]], axis=1) for o in range(chunk)
        ]
        rank = jnp.dot(jnp.concatenate(left, axis=0), prefix, preferred_element_type=F32)
        for o in range(chunk):
            base = ((step * chunk + o) * capacity) * 1.0
            place = jnp.where(masks[o], rank[o * rows : (o + 1) * rows] + base, place)
        return place

    place = jnp.zeros((rows, LANES), F32)
    if devices <= 4 * chunk:
        for step in range(devices // chunk):
            place = ranks(step, place)
    else:
        place = lax.fori_loop(0, devices // chunk, ranks, place)
    place_ref[...] = place.astype(jnp.int32)


def pack_nodes(first, last, place_ref, val_ref, acc_ref):
    wide = 2 * LANES
    groups = acc_ref.shape[0] // 3
    pair = 16
    group_id = exact_ids(groups, LANES)
    lane_id = exact_ids(wide, LANES)

    def spread(step, carry):
        columns, parts = [], [[] for _ in range(6)]
        for u in range(ROW_STEP):
            row = step * ROW_STEP + u
            at = place_ref[pl.ds(row, 1), :]
            hit = equal_hot(group_id, at // wide)
            columns.append(equal_hot(lane_id, at % wide))
            for c in range(3):
                value = val_ref[pl.ds(c, 1), pl.ds(pl.multiple_of(row * LANES, LANES), LANES)]
                value = jnp.broadcast_to(value, (pair, LANES))
                high = value.astype(BF16)
                low = (value - high.astype(F32)).astype(BF16)
                for n, part in ((c, high), (3 + c, low)):
                    parts[n].append(hit * jnp.concatenate([part] * (groups // pair), axis=0))
        left = jnp.concatenate([jnp.concatenate(part, axis=1) for part in parts], axis=0)
        right = jnp.concatenate(columns, axis=1)
        product = lax.dot_general(left, right, (((1,), (1,)), ((), ())), preferred_element_type=F32)
        acc_ref[...] += product[: 3 * groups] + product[3 * groups :]
        return carry

    lax.fori_loop(first, last, spread, 0)


def strips(num_struct, count_y, free):
    strip = free // num_struct + 2 * SWEEPS
    per_tile = LANES // strip
    return strip, per_tile, -(-num_struct * count_y // per_tile), -(-7 * count_y // per_tile)


def window_kernel(
    counts,
    shell,
    owner,
    slot,
    weight,
    prev,
    offset,
    split,
    out,
    v_shell,
    v_owner,
    v_slot,
    v_weight,
    v_prev,
    v_offset,
    v_split,
    place,
    acc,
    packed,
    received,
    both,
    v_wall,
    tiles,
    near_in,
    edge_in,
    wall_in,
    back_out,
    back_in,
    main_field,
    main_motion,
    main_grad,
    main_scale,
    edge_field,
    edge_motion,
    edge_grad,
    edge_scale,
    work,
    local_sem,
    near_send,
    near_recv,
    edge_send,
    edge_recv,
    pack_send,
    pack_recv,
    wall_send,
    wall_recv,
    back_send,
    back_recv,
):
    num_struct, num_fluid = counts
    devices = num_struct * num_fluid
    s, f = lax.axis_index("struct"), lax.axis_index("fluid")
    me = s * num_fluid + f
    stencil, count_y, count_z, wall = slot.shape
    free = prev.shape[3] - wall
    nodes = count_y * count_z
    deep = 2 * count_z
    span = count_y * COLUMNS
    share = free // num_struct
    rows_all = num_struct * count_y
    strip, per_tile, main_tiles, near_tiles = strips(num_struct, count_y, free)
    rows_own = v_owner.shape[0]
    capacity = 2 * rows_own * LANES // devices
    pieces = capacity // LANES
    groups = devices * pieces
    far_wall = 2 * SWEEPS + SWEEPS + 1

    def peer(ds, df):
        return ((s + ds + num_struct) % num_struct, (f + df + num_fluid) % num_fluid)

    def remote(src, dst, send, recv, where):
        return pltpu.make_async_remote_copy(
            src_ref=src, dst_ref=dst, send_sem=send, recv_sem=recv, device_id=where, device_id_type=MESH
        )

    loads = [
        (owner, v_owner),
        (offset, v_offset),
        (split, v_split),
        (prev.at[:, :, :, pl.ds(wall, free)], v_prev),
        (shell, v_shell),
        (slot, v_slot),
        (weight, v_weight),
    ]
    loads = [pltpu.make_async_copy(a, b, local_sem.at[n]) for n, (a, b) in enumerate(loads)]
    for load in loads:
        load.start()

    barrier = pltpu.get_barrier_semaphore()

    shifts = sorted(range(num_fluid), key=lambda d: -min(d, num_fluid - d))
    everyone = [peer(ds, df) for ds in range(num_struct) for df in shifts if (ds, df) != (0, 0)]
    for to in everyone:
        pl.semaphore_signal(barrier, inc=1, device_id=to, device_id_type=MESH)

    acc[...] = jnp.zeros_like(acc)
    with jax.named_scope("place"):
        loads[0].wait()
        place_nodes(devices, capacity, v_owner, place)

    lane = iota((count_z, LANES), 1)
    with jax.named_scope("tiles"):
        for load in loads[1:4]:
            load.wait()
        slab = jnp.zeros((count_z, LANES), F32)
        joined = [[None] * near_tiles for _ in range(num_struct)]
        for n in range(7):
            for j in range(count_y):
                if n < 3:
                    near, far = v_offset[n, j, :, :wall], v_offset[n, j, :, wall:]
                elif n == 3:
                    near, far = v_split[j, :, :wall].astype(F32), v_split[j, :, wall:].astype(F32)
                else:
                    near, far = jnp.zeros((count_z, LANES), F32), v_prev[n - 4, j]
                for q in range(num_struct):
                    begin = share * q - SWEEPS
                    line = far
                    if begin < 0:
                        line = jnp.where(lane >= LANES + begin, near, far)
                    if begin + strip > LANES:
                        line = jnp.where(lane < begin + strip - LANES, near, far)
                    t, m = divmod(n * count_y + j, per_tile)
                    line = turn(line, strip * m - begin, 1)
                    joined[q][t] = jnp.where(lane >= strip * m, line, joined[q][t]) if m else line
                if n < 4:
                    base = span * n + COLUMNS * j
                    low = turn(jnp.where(lane == LANES - 1, near, far), base + 1, 1)
                    high = turn(jnp.where(lane == 0, near, far), base + far_wall, 1)
                    slab = jnp.where((lane >= base) & (lane < base + 2 * SWEEPS), low, slab)
                    slab = jnp.where(
                        (lane >= base + 2 * SWEEPS) & (lane < base + COLUMNS), high, slab
                    )
        for q in range(num_struct):
            for t in range(near_tiles):
                tiles[q, t] = joined[q][t]
        edge_in[0] = slab

    with jax.named_scope("pack"):
        loads[4].wait()
        pack_nodes(0, rows_own // ROW_STEP, place, v_shell, acc)
    with jax.named_scope("relay"):
        pack_groups = groups // 2
        for o in range(devices):
            for c in range(3):
                for b in range(pieces):
                    m = o * pieces + b
                    packed[o, pl.ds(c * pieces + b, 1), :] = acc[
                        pl.ds(c * pack_groups + m // 2, 1), pl.ds((m % 2) * LANES, LANES)
                    ]
    with jax.named_scope("barrier"):
        pl.semaphore_wait(barrier, devices - 1)

    around = [(r, df) for df in (-1, 1, 0) for r in range(num_struct) if (r, df) != (0, 0)]

    def planes_of(df):
        return pl.ds(0, count_z) if df == 0 else pl.ds(0 if df > 0 else SWEEPS, SWEEPS)

    def near_copy(r, df):
        to = peer(-r, -df)
        return remote(
            tiles.at[to[0], :, planes_of(df)],
            near_in.at[2 * r + (df != 0), :, planes_of(df)],
            near_send,
            near_recv,
            to,
        )

    others = pl.ds(1, 2 * num_struct - 1)
    def spread_copy(buffer, send, recv, r, df):
        return remote(
            buffer.at[0, planes_of(df)],
            buffer.at[2 * r + (df != 0), planes_of(df)],
            send,
            recv,
            peer(-r, -df),
        )

    def send_around(buffer, send, recv):
        for r, df in around:
            spread_copy(buffer, send, recv, r, df).start()
        return remote(buffer.at[others], buffer.at[others], send, recv, peer(1, 0))

    all_edges = send_around(edge_in, edge_send, edge_recv)
    for r, df in around:
        near_copy(r, df).start()
    all_near = remote(near_in.at[others], near_in.at[others], near_send, near_recv, peer(1, 0))
    near_in[0] = tiles[s]


    with jax.named_scope("sendpack"):

        for to in everyone:
            remote(packed.at[to[0] * num_fluid + to[1]], received.at[me], pack_send, pack_recv, to).start()
        received[me] = packed[me]
    all_packs = remote(
        packed.at[pl.ds(0, devices - 1)],
        received.at[pl.ds(0, devices - 1)],
        pack_send,
        pack_recv,
        peer(1, 0),
    )

    lane_deep = iota((deep, LANES), 1)
    column = lane_deep % strip + share * s
    within = lane_deep % COLUMNS
    inner = ((within >= 1) & (within <= SWEEPS)) | ((within > 2 * SWEEPS) & (within < far_wall))
    free_node = (column >= SWEEPS) & (column < free + SWEEPS) & (lane_deep < strip * per_tile)

    tail = [strip * (min(per_tile, rows_all - per_tile * t) - 1) for t in range(main_tiles)]

    def main_corners(read):
        values = [[read(t, c) for c in range(3)] for t in range(main_tiles)]
        for t, here in enumerate(values):
            following = values[(t + 1) % main_tiles]
            high = [
                [
                    jnp.where(lane_deep < tail[t], turn(p, -strip - a, 1), turn(q, tail[t] - a, 1))
                    for p, q in zip(here, following)
                ]
                for a in (0, 1)
            ]
            near = [turn(p, -1, 1) for p in here]
            yield t, with_planes({(0, 0): here, (1, 0): near, (0, 1): high[0], (1, 1): high[1]})

    def main_sums():
        lows, insides, outsides = [], [], []
        for t in range(main_tiles):
            ends = close_cells(work.at[t], float_codes(main_field[t, 3]))
            lows.append([p + turn(q, 1, 1) for p, q in zip(ends[0, 0], ends[1, 0])])
            upper = list(zip(ends[0, 1], ends[1, 1]))
            insides.append([turn(p, strip, 1) + turn(q, strip + 1, 1) for p, q in upper])
            outsides.append([turn(p, -tail[t], 1) + turn(q, 1 - tail[t], 1) for p, q in upper])
        for t in range(main_tiles):
            yield t, [
                p + jnp.where(lane_deep < strip, before, now)
                for p, before, now in zip(lows[t], outsides[t - 1], insides[t])
            ]

    def prepare_main():
        source = [
            [jnp.concatenate([near_in[2 * r, t], near_in[2 * r + 1, t]], axis=0) for t in range(near_tiles)]
            for r in range(num_struct)
        ]
        for n in range(7):
            for t in range(main_tiles):
                total = None
                for m in range(min(per_tile, rows_all - per_tile * t)):
                    r, j = divmod(per_tile * t + m, count_y)
                    k, at = divmod(n * count_y + j, per_tile)
                    moved = turn(source[r][k], strip * (m - at), 1)
                    total = jnp.where(lane_deep >= strip * m, moved, total) if m else moved
                if n < 4:
                    main_field[t, n] = total
                else:
                    main_motion[t, n - 4] = total
        for r, corners in main_corners(lambda at, c: main_field[at, c]):
            open_gradients(corners, float_codes(main_field[r, 3]), work.at[r])

        def row(r, carry):
            def put(n, rows, value):
                main_grad[r, n, rows] = value

            fill_gradients(work.at[r], put)
            return carry

        lax.fori_loop(0, main_tiles, row, 0)
        for r, values in main_sums():
            for c in range(3):
                main_scale[r, c] = jnp.where(free_node, RELAX_FACTOR / values[c], 0.0)

    def sweep_main(sweep, carry):
        for r, corners in main_corners(lambda at, c: main_motion[at, c]):
            open_forces(corners, float_codes(main_field[r, 3]), work.at[r])

        for r in range(main_tiles):
            fill_forces(lambda n, rows: main_grad[r, n, rows], work.at[r])
        for r, values in main_sums():
            for c in range(3):
                main_motion[r, c] = main_motion[r, c] - main_scale[r, c] * values[c]
        return carry

    def edge_corners(read):
        values = [read(c) for c in range(3)]
        return with_planes(
            {(a, b): [turn(p, -a - COLUMNS * b, 1) for p in values] for a in (0, 1) for b in (0, 1)}
        )

    def edge_sums():
        ends = close_cells(work.at[0], float_codes(edge_field[3]))
        moved = [[turn(p, a + COLUMNS * b, 1) for p in ends[a, b]] for a in (0, 1) for b in (0, 1)]
        return [(p + q) + (u + v) for p, q, u, v in zip(*moved)]

    def prepare_edge():
        for r in range(num_struct):
            whole = jnp.concatenate([edge_in[2 * r], edge_in[2 * r + 1]], axis=0)
            for n in range(4):
                moved = turn(whole, span * (r - n), 1)
                if r > 0:
                    moved = jnp.where(lane_deep >= span * r, moved, edge_field[n])
                edge_field[n] = moved
        open_gradients(edge_corners(lambda c: edge_field[c]), float_codes(edge_field[3]), work.at[0])

        def put(n, rows, value):
            edge_grad[n, rows] = value

        fill_gradients(work.at[0], put)
        for c, value in enumerate(edge_sums()):
            edge_scale[c] = jnp.where(inner, RELAX_FACTOR / value, 0.0)

    def plane_points(ref, zero):
        row, at = iota((nodes, LANES), 0), iota((nodes, LANES), 1)
        within = row // count_z * (2 * count_z) + count_z - 1 - row % count_z
        total = None
        for t in range(stencil):
            whole = jnp.concatenate([ref[t, j] for j in range(count_y)], axis=0)
            for side in (0, 1):
                edge = wall - 1 if side == 0 else 0
                spread = jnp.broadcast_to(whole[:, edge : edge + 1], (nodes, LANES))
                part = jnp.where(at == 2 * nodes * t + count_z * side + within, spread, zero)
                total = part if total is None else total + part
        return jnp.sum(total, axis=0, keepdims=True)

    with jax.named_scope("prepedge"):
        all_edges.wait_recv()
        prepare_edge()
    with jax.named_scope("points"):
        loads[5].wait()
        loads[6].wait()
        plane_slot, plane_weight = plane_points(v_slot, 0), plane_points(v_weight, 0.0)

    with jax.named_scope("waitnear"):
        all_near.wait_recv()
    with jax.named_scope("prepmain"):
        prepare_main()
    with jax.named_scope("sweeps"):
        lax.fori_loop(0, EARLY_SWEEPS, sweep_main, 0)
    with jax.named_scope("waitpack"):
        all_packs.wait_recv()

    with jax.named_scope("table"):
        for c in range(3):
            whole = jnp.concatenate(
                [received[o, pl.ds(c * pieces, pieces), :] for o in range(devices)], axis=0
            )
            high, low = split_two(whole)
            both[pl.ds(c * groups, groups), :LANES] = high
            both[pl.ds(c * groups, groups), LANES:] = low

    with jax.named_scope("planes"):
        pick = one_hot(iota((LANES, LANES), 0) == plane_slot % LANES)
        found = jnp.dot(both[...], jnp.concatenate([pick, pick], axis=0), preferred_element_type=F32)
        scaled = jnp.where(iota((groups, LANES), 0) == plane_slot // LANES, plane_weight, 0.0)
        tile = jnp.zeros((count_z, LANES), F32)
        for c in range(3):
            line = jnp.sum(found[c * groups : (c + 1) * groups] * scaled, axis=0, keepdims=True)
            period = LANES // 2
            while period >= 2 * nodes:
                line = line + turn(line, period, 1)
                period //= 2
            spread = pltpu.roll(jnp.broadcast_to(line, (count_z, LANES)), 0, 1, stride=1, stride_axis=0)
            tile = jnp.where((lane >= span * c) & (lane < span * (c + 1)), spread, tile)
        wall_in[0] = tile

    all_walls = send_around(wall_in, wall_send, wall_recv)

    with jax.named_scope("latesweeps"):
        lax.fori_loop(EARLY_SWEEPS, SWEEPS, sweep_main, 0)

    def send_back():
        for r in range(num_struct):
            for c in range(3):
                total = None
                for j in range(count_y):
                    t, m = divmod(r * count_y + j, per_tile)
                    moved = turn(main_motion[t, c, :count_z, :], strip * (j - m), 1)
                    total = jnp.where(lane >= strip * j, moved, total) if j else moved
                back_out[r, c] = total
        for r in range(1, num_struct):
            remote(back_out.at[r], back_in.at[s], back_send, back_recv, peer(r, 0)).start()
        back_in[s] = back_out[0]

    strangers = pl.ds(0, num_struct - 1)
    all_back = remote(back_in.at[strangers], back_in.at[strangers], back_send, back_recv, peer(1, 0))
    send_back()
    wide = 2 * LANES
    lane_id = exact_ids(LANES, wide)
    group_id = iota((groups, wide), 0)

    def pair(step):
        j, k = 2 * step // count_z, 2 * step % count_z
        sums = [None] * 3
        for t in range(stencil):
            at = jnp.concatenate(
                [v_slot[t, j, pl.ds(k, 1), :], v_slot[t, j, pl.ds(k + 1, 1), :]], axis=1
            )
            by = jnp.concatenate(
                [v_weight[t, j, pl.ds(k, 1), :], v_weight[t, j, pl.ds(k + 1, 1), :]], axis=1
            )
            choose = equal_hot(lane_id, at % LANES)
            values = jnp.dot(
                both[...], jnp.concatenate([choose, choose], axis=0), preferred_element_type=F32
            )
            factor = jnp.where(group_id == at // LANES, by, 0.0)
            for c in range(3):
                term = values[c * groups : (c + 1) * groups] * factor
                sums[c] = term if sums[c] is None else sums[c] + term
        for c in range(3):
            line = jnp.sum(sums[c], axis=0, keepdims=True)
            v_wall[c, pl.ds(2 * step, 1), :] = line[:, :LANES]
            v_wall[c, pl.ds(2 * step + 1, 1), :] = line[:, LANES:]

    def pairs(step, carry):
        for u in range(WALL_STEP):
            pair(step * WALL_STEP + u)
        return carry

    with jax.named_scope("wall"):
        lax.fori_loop(0, nodes // 2 // WALL_STEP, pairs, 0)

    with jax.named_scope("waitwall"):
        all_walls.wait_recv()
    with jax.named_scope("edgeinit"):
        arrived = [jnp.concatenate([wall_in[2 * r], wall_in[2 * r + 1]], axis=0) for r in range(num_struct)]
        for c in range(3):
            total = jnp.zeros((deep, LANES), F32)
            for r in range(num_struct):
                here = lane_deep // span == r
                shift = span * (r - c) - (count_z - 1)
                total = jnp.where(here & (within == 0), turn(arrived[r], shift, 1), total)
                shift = shift - count_z + far_wall
                total = jnp.where(here & (within == far_wall), turn(arrived[r], shift, 1), total)
            edge_motion[c] = total

    def sweep_edge(step, carry):
        open_forces(edge_corners(lambda c: edge_motion[c]), float_codes(edge_field[3]), work.at[0])
        fill_forces(lambda n, rows: edge_grad[n, rows], work.at[0])
        for c, value in enumerate(edge_sums()):
            edge_motion[c] = edge_motion[c] - edge_scale[c] * value
        return carry

    with jax.named_scope("sweepedge"):
        lax.fori_loop(0, SWEEPS, sweep_edge, 0)

    with jax.named_scope("waitback"):
        all_back.wait_recv()
    with jax.named_scope("outs"):
        for c in range(3):
            for j in range(count_y):
                out[c, j, :, :wall] = v_wall[c, pl.ds(j * count_z, count_z), :]
                total = None
                for q in range(num_struct):
                    moved = turn(back_in[q, c], share * q - strip * j - SWEEPS, 1)
                    total = moved if total is None else jnp.where(lane >= share * q, moved, total)
                delta = edge_motion[c, :count_z, :]
                low = turn(delta, -1 - COLUMNS * j, 1)
                high = turn(delta, free - far_wall - COLUMNS * j, 1)
                change = jnp.where(lane < SWEEPS, low, jnp.where(lane >= free - SWEEPS, high, 0.0))
                out[c, j, :, wall:] = total + change

    with jax.named_scope("waitsend"):
        for group in (all_near, all_edges, all_walls, all_back, all_packs):
            group.wait_send()


def shards(shell_motion, owner, stencil_slot, stencil_weight, prev_motion, node_offset, cell_split):
    num_struct, num_fluid = lax.axis_size("struct"), lax.axis_size("fluid")
    devices = num_struct * num_fluid
    own = shell_motion.shape[1]
    pieces = 2 * own // devices // LANES
    groups = devices * pieces
    stencil, count_y, count_z, wall = stencil_slot.shape
    total_x = prev_motion.shape[3]
    free = total_x - wall
    nodes, deep = count_y * count_z, 2 * count_z
    assert wall == free == LANES and count_z == 2 * SWEEPS == 8 and num_struct >= 2 and num_fluid >= 3
    assert num_struct * count_y * COLUMNS == LANES and 2 * stencil * nodes == LANES
    strip, per_tile, main_tiles, near_tiles = strips(num_struct, count_y, free)
    assert count_y <= per_tile and num_struct * count_y > per_tile
    vmem, dma = pltpu.VMEM, pltpu.SemaphoreType.DMA
    scratch = [
        vmem((3, own), F32),
        vmem((own // LANES, LANES), jnp.int32),
        vmem((stencil, count_y, count_z, wall), jnp.int32),
        vmem((stencil, count_y, count_z, wall), F32),
        vmem((3, count_y, count_z, free), F32),
        vmem((3, count_y, count_z, total_x), F32),
        vmem((count_y, count_z, total_x), jnp.int32),
        vmem((own // LANES, LANES), jnp.int32),
        vmem((3 * groups // 2, 2 * LANES), F32),
        vmem((devices, 3 * pieces, LANES), F32),
        vmem((devices, 3 * pieces, LANES), F32),
        vmem((3 * groups, 2 * LANES), BF16),
        vmem((3, nodes, wall), F32),
        vmem((num_struct, near_tiles, count_z, LANES), F32),
        vmem((2 * num_struct, near_tiles, count_z, LANES), F32),
        vmem((2 * num_struct, count_z, LANES), F32),
        vmem((2 * num_struct, count_z, LANES), F32),
        vmem((num_struct, 3, count_z, LANES), F32),
        vmem((num_struct, 3, count_z, LANES), F32),
        vmem((main_tiles, 4, deep, LANES), F32),
        vmem((main_tiles, 3, deep, LANES), F32),
        vmem((main_tiles, 54, deep, LANES), F32),
        vmem((main_tiles, 3, deep, LANES), F32),
        vmem((4, deep, LANES), F32),
        vmem((3, deep, LANES), F32),
        vmem((54, deep, LANES), F32),
        vmem((3, deep, LANES), F32),
        vmem((main_tiles, 2, 24, deep, LANES), F32),
        dma((7,)),
        dma,
        dma,
        dma,
        dma,
        dma,
        dma,
        dma,
        dma,
        dma,
        dma,
    ]
    return pl.pallas_call(
        functools.partial(window_kernel, (num_struct, num_fluid)),
        out_shape=pltpu.VMEM(prev_motion.shape, F32),
        in_specs=[pl.BlockSpec(memory_space=pltpu.HBM)] * 7,
        out_specs=pl.BlockSpec(memory_space=pltpu.VMEM),
        scratch_shapes=scratch,
        cost_estimate=pl.CostEstimate(flops=4 << 30, bytes_accessed=16 << 20, transcendentals=0),
        compiler_params=pltpu.CompilerParams(
            collective_id=0, has_side_effects=True, vmem_limit_bytes=67043328 - (1 << 17)
        ),
    )(
        shell_motion,
        owner.reshape(own // LANES, LANES),
        stencil_slot,
        stencil_weight,
        prev_motion,
        node_offset,
        cell_split,
    )


def solution(mesh):
    return jax.shard_map(
        shards,
        mesh=mesh,
        in_specs=(
            P(None, ("struct", "fluid")),
            P(("struct", "fluid"), None),
            P(None, "struct", "fluid", None),
            P(None, "struct", "fluid", None),
            P(None, "struct", "fluid", None),
            P(None, "struct", "fluid", None),
            P("struct", "fluid", None),
        ),
        out_specs=P(None, "struct", "fluid", None),
        check_vma=False,
    )
```
